16 devices in a mesh: dp: 2 (over y, z), cp: 8 (over x, core).
Axes of the slice: x: 4, y: 2, z: 1, core: 2. Of those that a mesh axis runs over, the one named last changes fastest.
The devices are a block of a 4x4x8 slice.
Arguments:
- x_in: bfloat16 [1024, 2048], P(('dp', 'cp')), parts along dimension 0
- cache_k1: bfloat16 [32768, 2, 128], P(('dp', 'cp')), parts along dimension 0
- cache_v1: bfloat16 [32768, 2, 128], P(('dp', 'cp')), parts along dimension 0
- w_q1: bfloat16 [2048, 2048], replicated
- b_q1: bfloat16 [2048], replicated
- w_k1: bfloat16 [2048, 256], replicated
- b_k1: bfloat16 [256], replicated
- w_v1: bfloat16 [2048, 256], replicated
- w_o1: bfloat16 [2048, 2048], replicated
- w_gate: bfloat16 [2048, 11008], replicated
- w_up: bfloat16 [2048, 11008], replicated
- w_down: bfloat16 [11008, 2048], replicated
- cache_k2: bfloat16 [32768, 2, 128], P(('dp', 'cp')), parts along dimension 0
- cache_v2: bfloat16 [32768, 2, 128], P(('dp', 'cp')), parts along dimension 0
- w_q2: bfloat16 [2048, 2048], replicated
- b_q2: bfloat16 [2048], replicated
- w_k2: bfloat16 [2048, 256], replicated
- b_k2: bfloat16 [256], replicated
- w_v2: bfloat16 [2048, 256], replicated
- w_o2: bfloat16 [2048, 2048], replicated
Outputs:
- output 1: bfloat16 [1024, 2048], P(('dp', 'cp')), parts along dimension 0
- output 2: bfloat16 [1024, 2048], P(('dp', 'cp')), parts along dimension 0
- output 3: bfloat16 [1024, 2, 128], P(('dp', 'cp')), parts along dimension 0
- output 4: bfloat16 [1024, 2, 128], P(('dp', 'cp')), parts along dimension 0
- output 5: bfloat16 [1024, 2, 128], P(('dp', 'cp')), parts along dimension 0
- output 6: bfloat16 [1024, 2, 128], P(('dp', 'cp')), parts along dimension 0
There are 2 independent parts. The reference program is written for one: setup_inputs(seed, part) draws one part's arguments, and reference() takes and returns one part's arrays. A program takes and returns all parts, laid end to end along the dimension named above; an argument that names none is the same for every part.
All inputs are finite; a program needn't handle non-finite values.
Results may differ from the reference program's by a relative error of at most 0.0144509.
Values are sent between devices in bfloat16 or wider.
A program may use at most 768 MiB of HBM per device.

```python
import math
import jax
import jax.numpy as jnp
from jax import lax

D_MODEL = 2048
HEADS = 16
KV_HEADS = 2
HEAD = 128
FF = 11008
CHUNK = 512
CACHE = 16384
SHARDS = 8
QBLK = 64

GROUP = HEADS // KV_HEADS
SHARD_LEN = CACHE // SHARDS


def draw_matrix(key, rows, cols):
    return (jax.random.normal(key, (rows, cols), jnp.float32) * rows ** -0.5).astype(jnp.bfloat16)


def draw_cache(key_k, key_s, key_v, key_m):
    shard_scale = jax.random.uniform(key_s, (SHARDS, 1, 1, 1), jnp.float32, 0.6, 1.6)
    cache_keys = jax.random.normal(key_k, (SHARDS, SHARD_LEN, KV_HEADS, HEAD), jnp.float32) * shard_scale
    shard_mean = jax.random.normal(key_m, (SHARDS, 1, KV_HEADS, HEAD), jnp.float32)
    cache_vals = 0.5 * jax.random.normal(key_v, (SHARDS, SHARD_LEN, KV_HEADS, HEAD), jnp.float32) + shard_mean
    return (cache_keys.reshape(CACHE, KV_HEADS, HEAD).astype(jnp.bfloat16),
            cache_vals.reshape(CACHE, KV_HEADS, HEAD).astype(jnp.bfloat16))


def draw_bias(key_dir, key_q, key_k):
    half_dim = HEAD // 2
    lane_idx = jnp.arange(HEAD) % half_dim
    low_mask = (lane_idx >= (7 * half_dim) // 8).astype(jnp.float32)
    raw_dir = jax.random.normal(key_dir, (KV_HEADS, HEAD), jnp.float32) * low_mask
    unit_dir = raw_dir / jnp.sqrt(jnp.sum(raw_dir * raw_dir, axis=-1, keepdims=True))
    mean_score = max(math.log(CACHE / CHUNK) + 0.5, 0.5)
    bias_amp = math.sqrt(mean_score * math.sqrt(HEAD))
    jitter_q = jax.random.uniform(key_q, (HEADS, 1), jnp.float32, 0.9, 1.1)
    jitter_k = jax.random.uniform(key_k, (KV_HEADS, 1), jnp.float32, 0.9, 1.1)
    bias_q = bias_amp * jnp.repeat(unit_dir, GROUP, axis=0) * jitter_q
    bias_k = bias_amp * unit_dir * jitter_k
    return (bias_q.reshape(HEADS * HEAD).astype(jnp.bfloat16),
            bias_k.reshape(KV_HEADS * HEAD).astype(jnp.bfloat16))


def setup_inputs(seed: int = 0, part: int = 0) -> dict:
    shared_root, part_root = jax.random.split(jax.random.key(seed))
    part_keys = jax.random.split(jax.random.fold_in(part_root, part), 9)
    weight_keys = jax.random.split(shared_root, 17)
    x_in = jax.random.normal(part_keys[0], (CHUNK, D_MODEL), jnp.float32).astype(jnp.bfloat16)
    cache_k1, cache_v1 = draw_cache(part_keys[1], part_keys[2], part_keys[3], part_keys[4])
    cache_k2, cache_v2 = draw_cache(part_keys[5], part_keys[6], part_keys[7], part_keys[8])
    b_q1, b_k1 = draw_bias(weight_keys[0], weight_keys[1], weight_keys[2])
    b_q2, b_k2 = draw_bias(weight_keys[3], weight_keys[4], weight_keys[5])
    return {
        'x_in': x_in,
        'cache_k1': cache_k1,
        'cache_v1': cache_v1,
        'w_q1': draw_matrix(weight_keys[6], D_MODEL, HEADS * HEAD),
        'b_q1': b_q1,
        'w_k1': draw_matrix(weight_keys[7], D_MODEL, KV_HEADS * HEAD),
        'b_k1': b_k1,
        'w_v1': draw_matrix(weight_keys[8], D_MODEL, KV_HEADS * HEAD),
        'w_o1': draw_matrix(weight_keys[9], HEADS * HEAD, D_MODEL),
        'w_gate': draw_matrix(weight_keys[10], D_MODEL, FF),
        'w_up': draw_matrix(weight_keys[11], D_MODEL, FF),
        'w_down': draw_matrix(weight_keys[12], FF, D_MODEL),
        'cache_k2': cache_k2,
        'cache_v2': cache_v2,
        'w_q2': draw_matrix(weight_keys[13], D_MODEL, HEADS * HEAD),
        'b_q2': b_q2,
        'w_k2': draw_matrix(weight_keys[14], D_MODEL, KV_HEADS * HEAD),
        'b_k2': b_k2,
        'w_v2': draw_matrix(weight_keys[15], D_MODEL, KV_HEADS * HEAD),
        'w_o2': draw_matrix(weight_keys[16], HEADS * HEAD, D_MODEL),
    }


def rms_norm(vals):
    wide = vals.astype(jnp.float32)
    return (wide * lax.rsqrt(jnp.mean(wide * wide, axis=-1, keepdims=True) + 1e-5)).astype(jnp.bfloat16)


def rope_tables(positions):
    half_dim = HEAD // 2
    inv_freq = 1.0 / (500000.0 ** (jnp.arange(half_dim, dtype=jnp.float32) * (2.0 / HEAD)))
    angles = positions.astype(jnp.float32)[:, None] * inv_freq[None, :]
    return jnp.cos(angles)[:, None, :], jnp.sin(angles)[:, None, :]


def apply_rope(vals, cos_t, sin_t):
    half_dim = HEAD // 2
    first = vals[..., :half_dim]
    second = vals[..., half_dim:]
    return jnp.concatenate([first * cos_t - second * sin_t, second * cos_t + first * sin_t], axis=-1)


def attention_layer(layer_in, cache_k, cache_v, w_q, b_q, w_k, b_k, w_v, w_o):
    cos_t, sin_t = rope_tables(CACHE + jnp.arange(CHUNK))
    q_pre = (jnp.dot(layer_in, w_q, preferred_element_type=jnp.float32) + b_q.astype(jnp.float32)).astype(jnp.bfloat16)
    k_pre = (jnp.dot(layer_in, w_k, preferred_element_type=jnp.float32) + b_k.astype(jnp.float32)).astype(jnp.bfloat16)
    v_new = jnp.dot(layer_in, w_v, preferred_element_type=jnp.float32).astype(jnp.bfloat16).reshape(CHUNK, KV_HEADS, HEAD)
    q_rot = apply_rope(q_pre.reshape(CHUNK, HEADS, HEAD).astype(jnp.float32), cos_t, sin_t).astype(jnp.bfloat16)
    k_new = apply_rope(k_pre.reshape(CHUNK, KV_HEADS, HEAD).astype(jnp.float32), cos_t, sin_t).astype(jnp.bfloat16)
    keys_all = jnp.concatenate([cache_k, k_new], axis=0).astype(jnp.float32)
    vals_all = jnp.concatenate([cache_v, v_new], axis=0).astype(jnp.float32)
    key_pos = jnp.arange(CACHE + CHUNK)
    scale = HEAD ** -0.5
    q_blocks = q_rot.reshape(CHUNK // QBLK, QBLK, KV_HEADS, GROUP, HEAD)
    starts = jnp.arange(CHUNK // QBLK) * QBLK

    def one_block(blk_in):
        q_blk, start = blk_in
        scores = jnp.einsum('tkgd,skd->tkgs', q_blk.astype(jnp.float32), keys_all) * scale
        q_pos = CACHE + start + jnp.arange(QBLK)
        visible = key_pos[None, :] <= q_pos[:, None]
        scores = jnp.where(visible[:, None, None, :], scores, -jnp.inf)
        peak = jnp.max(scores, axis=-1, keepdims=True)
        prob_w = jnp.exp(scores - peak)
        total = jnp.sum(prob_w, axis=-1, keepdims=True)
        summed = jnp.einsum('tkgs,skd->tkgd', prob_w.astype(jnp.bfloat16).astype(jnp.float32), vals_all)
        return summed / total

    o_all = lax.map(one_block, (q_blocks, starts))
    o_half = o_all.reshape(CHUNK, HEADS * HEAD).astype(jnp.bfloat16)
    y_out = jnp.dot(o_half, w_o, preferred_element_type=jnp.float32).astype(jnp.bfloat16)
    return y_out, k_new, v_new


def reference(x_in, cache_k1, cache_v1, w_q1, b_q1, w_k1, b_k1, w_v1, w_o1, w_gate, w_up, w_down, cache_k2, cache_v2, w_q2, b_q2, w_k2, b_k2, w_v2, w_o2):
    y_one, k_one, v_one = attention_layer(x_in, cache_k1, cache_v1, w_q1, b_q1, w_k1, b_k1, w_v1, w_o1)
    resid_h = (x_in.astype(jnp.float32) + y_one.astype(jnp.float32)).astype(jnp.bfloat16)
    normed = rms_norm(resid_h)
    gate_act = jnp.dot(normed, w_gate, preferred_element_type=jnp.float32).astype(jnp.bfloat16)
    up_proj = jnp.dot(normed, w_up, preferred_element_type=jnp.float32).astype(jnp.bfloat16)
    mixed = (jax.nn.silu(gate_act.astype(jnp.float32)) * up_proj.astype(jnp.float32)).astype(jnp.bfloat16)
    hidden = (resid_h.astype(jnp.float32) + jnp.dot(mixed, w_down, preferred_element_type=jnp.float32)).astype(jnp.bfloat16)
    y_two, k_two, v_two = attention_layer(rms_norm(hidden), cache_k2, cache_v2, w_q2, b_q2, w_k2, b_k2, w_v2, w_o2)
    return (hidden, y_two, k_one, v_one, k_two, v_two)
```

```python
import functools
import math

import jax
import jax.numpy as jnp
import numpy as np
from jax import lax
from jax.experimental import pallas as pl
from jax.experimental.pallas import tpu as pltpu
from jax.sharding import PartitionSpec as P

ROPE_THETA = 500000.0
NORM_EPS = 1e-5
MESH = pl.DeviceIdType.MESH
F32 = jnp.float32
BF16 = jnp.bfloat16

ORDER = ("own0", "own1", "own2", "left0", "right1", "opp0", "opp1", "left2", "right3", "opp2", "opp3",
         "right0", "left1", "right2", "left3", "own3")
SLOT = {name: idx for idx, name in enumerate(ORDER)}
UNITS = len(ORDER)
PAIRS = 4
NORM_ROWS = 16


def rope_tables(first_pos, count, head_dim):
    half_dim = head_dim // 2
    exponent = np.arange(half_dim, dtype=np.float32) * np.float32(2.0 / head_dim)
    inv_freq = (np.float32(1.0) / np.power(np.float32(ROPE_THETA), exponent)).astype(np.float32)
    positions = (first_pos + np.arange(count)).astype(np.float32)
    angles = (positions[:, None] * inv_freq[None, :]).astype(np.float32)
    cos_t = np.cos(angles.astype(np.float64)).astype(np.float32)
    sin_t = np.sin(angles.astype(np.float64)).astype(np.float32)
    return np.concatenate([cos_t, cos_t], axis=1), np.concatenate([-sin_t, sin_t], axis=1)


def block_kernel(nchip, ff_chunk, ff_slots,
                 x_hbm, kc1, vc1, wq1, wk1, wv1, wo1, w_gate, w_up, w_down, kc2, vc2, wq2, wk2, wv2, wo2,
                 bias_ref, cos_hbm, sin_hbm,
                 g_out, y_out, k1_out, v1_out, k2_out, v2_out,
                 xbuf, hbuf, ubuf, wqb, wkb, wvb, wob, kall, vtall, kstage, vstage, ksend, vsend, deint,
                 qall, s_a, s_b, m_a, m_b, obuf, relay, final, ohalf, ysend, yrecv, macc, mrecv,
                 w1s, w3s, w2s, ebuf, cosb, sinb, kvout, gout,
                 dsem, rings, ssem, rsem):
    tok = x_hbm.shape[0]
    ctok = 2 * tok
    width = x_hbm.shape[1]
    hd = kc1.shape[1]
    keys_dev = kc1.shape[0] // 2
    keys_chip = 2 * keys_dev
    keys_tot = keys_chip + ctok
    rows = 2 * ctok
    half_w = width // 2
    ncol = 4
    cw = width // ncol
    cexp = math.log2(math.e) / math.sqrt(hd)

    me = lax.axis_index("cp")
    chip = me // 2
    core = lax.rem(me, 2)
    partner = chip * 2 + 1 - core
    left_chip = lax.rem(chip + nchip - 1, nchip)
    right_chip = lax.rem(chip + 1, nchip)
    opp_chip = lax.rem(chip + 2, nchip)
    left = left_chip * 2 + core
    right = right_chip * 2 + core

    dcount = [0]

    def local(src, dst):
        idx = dcount[0]
        dcount[0] += 1
        return pltpu.make_async_copy(src, dst, dsem.at[idx])

    rcount = [0]

    def remote(src, dst, dev):
        idx = rcount[0]
        rcount[0] += 1
        return pltpu.make_async_remote_copy(src_ref=src, dst_ref=dst, send_sem=ssem.at[idx], recv_sem=rsem.at[idx],
                                            device_id={"cp": dev}, device_id_type=MESH)

    barrier = pltpu.get_barrier_semaphore()
    for dev in (partner, left, right):
        pl.semaphore_signal(barrier, inc=1, device_id={"cp": dev}, device_id_type=MESH)

    my_rows = pl.ds(pl.multiple_of(core * tok, tok), tok)
    kc = (kc1, kc2)
    vc = (vc1, vc2)
    wq = (wq1, wq2)
    wk = (wk1, wk2)
    wv = (wv1, wv2)
    wo = (wo1, wo2)
    k_out = (k1_out, k2_out)
    v_out = (v1_out, v2_out)

    cp_x = local(x_hbm, xbuf.at[my_rows])
    pos_rows = pl.ds(pl.multiple_of(chip * ctok, ctok), ctok)
    cp_cos = local(cos_hbm.at[pos_rows], cosb)
    cp_sin = local(sin_hbm.at[pos_rows], sinb)
    cp_ks = [local(kc[la], kstage) for la in range(2)]
    cp_vs = [local(vc[la], vstage) for la in range(2)]
    qcol = [pl.ds(pl.multiple_of(core * half_w + hp * rows, rows), rows) for hp in range(PAIRS)]
    cp_wq = [[local(wq[la].at[:, qcol[hp]], wqb.at[hp]) for hp in range(PAIRS)] for la in range(2)]
    cp_wk = [local(wk[la], wkb) for la in range(2)]
    cp_wv = [local(wv[la], wvb) for la in range(2)]
    cp_wo = [local(wo[la].at[pl.ds(pl.multiple_of(core * half_w, half_w), half_w)], wob) for la in range(2)]
    cp_kout = [local(kvout.at[la, 0], k_out[la]) for la in range(2)]
    cp_vout = [local(kvout.at[la, 1], v_out[la]) for la in range(2)]
    cp_g = local(gout.at[0], g_out)
    cp_y = local(gout.at[1], y_out)

    rc_x = remote(x_hbm, xbuf.at[my_rows], partner)
    rc_k = [remote(ksend, kall.at[la, pl.ds(keys_dev, keys_dev)], partner) for la in range(2)]
    rc_v = [remote(vsend, vtall.at[la, :, pl.ds(keys_dev, keys_dev)], partner) for la in range(2)]
    rc_qr, rc_ql, rc_qf, rc_o = [], [], [], []
    for la in range(2):
        own = [qall.at[la, SLOT["own%d" % hp]] for hp in range(PAIRS)]
        rc_qr.append([remote(own[hp], qall.at[la, SLOT["left%d" % hp]], right) for hp in range(PAIRS)])
        rc_ql.append([remote(own[hp], qall.at[la, SLOT["right%d" % hp]], left) for hp in range(PAIRS)])
        fwd = []
        for hp in range(PAIRS):
            side, dev = ("left", right) if hp % 2 == 0 else ("right", left)
            fwd.append(remote(qall.at[la, SLOT["%s%d" % (side, hp)]], qall.at[la, SLOT["opp%d" % hp]], dev))
        rc_qf.append(fwd)
        outs = {}
        for hp in range(PAIRS):
            outs["left%d" % hp] = remote(obuf.at[SLOT["left%d" % hp]], final.at[la, 1, hp], left)
            outs["right%d" % hp] = remote(obuf.at[SLOT["right%d" % hp]], final.at[la, 0, hp], right)
            outs["opp%d" % hp] = remote(obuf.at[SLOT["opp%d" % hp]], relay.at[la, hp], right if hp % 2 == 0 else left)
        rc_o.append(outs)
    rc_y1 = [remote(ysend.at[n], yrecv.at[n], partner) for n in range(ncol)]
    other_rows = pl.ds(pl.multiple_of((1 - core) * tok, tok), tok)
    rc_y2 = [remote(ysend.at[n, other_rows], mrecv.at[n, pl.ds(ctok, tok)], partner) for n in range(ncol)]
    rc_m = [remote(macc.at[n], mrecv.at[n, pl.ds(0, ctok)], partner) for n in range(ncol)]

    ff_half = w_gate.shape[1] // 2
    nfull = ff_half // ff_chunk
    tail = ff_half - nfull * ff_chunk

    def ff_copies(chunk, slot, size):
        cols = pl.ds(pl.multiple_of(core * ff_half + chunk * ff_chunk, 128), size)
        return (pltpu.make_async_copy(w_gate.at[:, cols], w1s.at[slot, :, pl.ds(0, size)], rings.at[0, slot]),
                pltpu.make_async_copy(w_up.at[:, cols], w3s.at[slot, :, pl.ds(0, size)], rings.at[1, slot]),
                pltpu.make_async_copy(w_down.at[cols], w2s.at[slot, pl.ds(0, size)], rings.at[2, slot]))

    def rope(val, la_bias, cos_v, sin_v):
        val = (val + la_bias).astype(BF16).astype(F32)
        return (val * cos_v + pltpu.roll(val, hd // 2, 1) * sin_v).astype(BF16)

    def prep_cache(la):
        if la == 1:
            rc_k[0].wait_send()
            rc_v[0].wait_send()
        step_rows = 2 * hd

        def split(ref, i):
            deint[...] = ref[pl.ds(pl.multiple_of(i * step_rows, step_rows), step_rows), :].astype(F32)
            head0 = deint[pl.ds(0, hd, stride=2), :]
            head1 = deint[pl.ds(1, hd, stride=2), :]
            is0 = core == 0
            return jnp.where(is0, head0, head1), jnp.where(is0, head1, head0)

        def kbody(i, _):
            mine, other = split(kstage, i)
            at = pl.ds(pl.multiple_of(i * hd, hd), hd)
            kall[la, at, :] = mine.astype(BF16)
            ksend[at, :] = other.astype(BF16)
            return 0

        def vbody(i, _):
            mine, other = split(vstage, i)
            at = pl.ds(pl.multiple_of(i * hd, hd), hd)
            vtall[la, :, at] = mine.T.astype(BF16)
            vsend[:, at] = other.T.astype(BF16)
            return 0

        cp_ks[la].wait()
        lax.fori_loop(0, keys_dev // hd, kbody, 0)
        rc_k[la].start()
        cp_vs[la].wait()
        lax.fori_loop(0, keys_dev // hd, vbody, 0)
        rc_v[la].start()
        if la == 0:
            cp_ks[1].start()
            cp_vs[1].start()

    def project(la, in_ref):
        heads_all = wq1.shape[1] // hd
        base = la * (heads_all + 2)

        def bias_row(idx):
            return bias_ref[pl.ds(idx, 1), :]

        cos_v, sin_v = cosb[...], sinb[...]
        for hp in range(PAIRS):
            cp_wq[la][hp].wait()
            acc = jnp.dot(in_ref[...], wqb[hp], preferred_element_type=F32)
            slot = SLOT["own%d" % hp]
            for j in range(2):
                row = base + core * (heads_all // 2) + hp * 2 + j
                qall[la, slot, pl.ds(j * ctok, ctok), :] = rope(acc[:, j * hd:(j + 1) * hd], bias_row(row), cos_v, sin_v)
            rc_qr[la][hp].start()
            rc_ql[la][hp].start()
        cp_wk[la].wait()
        acc = jnp.dot(in_ref[...], wkb[...], preferred_element_type=F32)
        k_heads = [rope(acc[:, j * hd:(j + 1) * hd], bias_row(base + heads_all + j), cos_v, sin_v).astype(F32) for j in range(2)]
        cp_wv[la].wait()
        acc = jnp.dot(in_ref[...], wvb[...], preferred_element_type=F32)
        v_heads = [acc[:, j * hd:(j + 1) * hd].astype(BF16).astype(F32) for j in range(2)]
        is0 = core == 0
        kall[la, pl.ds(keys_chip, ctok), :] = jnp.where(is0, k_heads[0], k_heads[1]).astype(BF16)
        vtall[la, :, pl.ds(keys_chip, ctok)] = jnp.where(is0, v_heads[0], v_heads[1]).T.astype(BF16)
        for which, heads in ((0, k_heads), (1, v_heads)):
            for j in range(2):
                mine = jnp.where(is0, heads[j][:tok], heads[j][tok:])
                deint[pl.ds(j, tok, stride=2), :] = mine
            kvout[la, which] = deint[pl.ds(0, 2 * tok), :].astype(BF16)
        cp_kout[la].start()
        cp_vout[la].start()

    offs = {"own": 0, "left": (left_chip - chip) * ctok, "right": (right_chip - chip) * ctok, "opp": (opp_chip - chip) * ctok}

    def unit_offset(unit):
        res = jnp.int32(0)
        for name, idx in SLOT.items():
            if not name.startswith("own"):
                res = jnp.where(unit == idx, offs[name[:-1]], res)
        return res

    def scores(la, unit, s_ref, m_ref):
        s_val = lax.dot_general(kall[la], qall[la, unit], (((1,), (1,)), ((), ())), preferred_element_type=F32)
        s_ref[pl.ds(0, keys_chip), :] = s_val[:keys_chip]
        peak = jnp.max(s_val[:keys_chip].reshape(keys_chip // 8, 8, rows), axis=0)
        key_i = lax.broadcasted_iota(jnp.int32, (ctok, rows), 0)
        tok_i = lax.broadcasted_iota(jnp.int32, (ctok, rows), 1) % ctok
        masked = jnp.where(key_i - tok_i <= unit_offset(unit), s_val[keys_chip:], -jnp.inf)
        s_ref[pl.ds(keys_chip, ctok), :] = masked
        m_ref[...] = jnp.maximum(peak, jnp.max(masked.reshape(ctok // 8, 8, rows), axis=0))

    row8 = lax.broadcasted_iota(jnp.int32, (8, rows), 0)

    def put(dst, out_v, peak, total):
        dst[pl.ds(0, hd), :] = out_v
        dst[pl.ds(hd, 8), :] = jnp.where(row8 == 0, peak, total)

    def get(src):
        return src[pl.ds(0, hd), :], src[pl.ds(hd, 1), :], src[pl.ds(hd + 1, 1), :]

    def merged(parts):
        peak = functools.reduce(jnp.maximum, [part[1] for part in parts])
        scales = [jnp.exp2((part[1] - peak) * cexp) for part in parts]
        out_v = functools.reduce(jnp.add, [part[0] * sc for part, sc in zip(parts, scales)])
        total = functools.reduce(jnp.add, [part[2] * sc for part, sc in zip(parts, scales)])
        return out_v, peak, total

    def attend_unit(la, unit, nxt, s_cur, m_cur, s_nxt, m_nxt):
        peak = jnp.max(m_cur[...], axis=0, keepdims=True)
        shift = jnp.broadcast_to(peak * cexp, (8, rows))
        prob = jnp.exp2(s_cur[...].reshape(keys_tot // 8, 8, rows) * cexp - shift[None])
        total = jnp.sum(jnp.sum(prob, axis=0), axis=0, keepdims=True)
        out_v = jnp.dot(vtall[la], prob.reshape(keys_tot, rows).astype(BF16), preferred_element_type=F32)
        scores(la, nxt, s_nxt, m_nxt)
        put(obuf.at[unit], out_v, peak, total)

    def before(la):
        acts = {}

        def add(name, *fns):
            acts.setdefault(SLOT[name] - 1, []).extend(fns)

        for hp in range(PAIRS):
            lw, rw = rc_qr[la][hp].wait_recv, rc_ql[la][hp].wait_recv
            fwd = rc_qf[la][hp]
            if hp % 2 == 0:
                acts.setdefault(2 if hp == 0 else 4, []).extend([lw, fwd.start])
                add("right%d" % hp, rw)
            else:
                acts.setdefault(3 if hp == 1 else 5, []).extend([rw, fwd.start])
                add("left%d" % hp, lw)
        for hp in range(PAIRS):
            add("opp%d" % hp, rc_qf[la][hp].wait_recv)
        return acts

    def after(la):
        acts = {}
        for name, cp in rc_o[la].items():
            hp = int(name[-1])
            merge_it = (name.startswith("right") and hp % 2 == 0) or (name.startswith("left") and hp % 2 == 1)

            def act(name=name, cp=cp, hp=hp, merge_it=merge_it):
                if merge_it:
                    rc_o[la]["opp%d" % hp].wait_recv()
                    put(obuf.at[SLOT[name]], *merged([get(obuf.at[SLOT[name]]), get(relay.at[la, hp])]))
                cp.start()

            acts[SLOT[name]] = [act]
        return acts

    def attention(la):
        rc_k[la].wait_recv()
        rc_v[la].wait_recv()
        scores(la, 0, s_a, m_a)
        pre, post = before(la), after(la)

        def run(acts, pair, parity):
            for unit, fns in acts.items():
                if unit % 2 == parity:
                    @pl.when(pair == unit // 2)
                    def _(fns=fns):
                        for fn in fns:
                            fn()

        def body(pair, _):
            run(pre, pair, 0)
            attend_unit(la, 2 * pair, 2 * pair + 1, s_a, m_a, s_b, m_b)
            run(post, pair, 0)
            run(pre, pair, 1)
            attend_unit(la, 2 * pair + 1, jnp.minimum(2 * pair + 2, UNITS - 1), s_b, m_b, s_a, m_a)
            run(post, pair, 1)
            return 0

        lax.fori_loop(0, UNITS // 2, body, 0)

    def finish_attention(la):
        for hp in range(PAIRS):
            rc_o[la]["right%d" % hp].wait_recv()
            rc_o[la]["left%d" % hp].wait_recv()
            out_v, _, total = merged([get(obuf.at[SLOT["own%d" % hp]]), get(final.at[la, 0, hp]), get(final.at[la, 1, hp])])
            out_v = out_v / total
            for j in range(2):
                ohalf[:, pl.ds((2 * hp + j) * hd, hd)] = out_v[:, j * ctok:(j + 1) * ctok].T.astype(BF16)
        cp_wo[la].wait()
        rc_y = (rc_y1, rc_y2)[la]
        for n in range(ncol):
            ysend[n] = jnp.dot(ohalf[...], wob[:, n * cw:(n + 1) * cw], preferred_element_type=F32)
            rc_y[n].start()
        for cp in list(rc_qr[la]) + list(rc_ql[la]) + list(rc_qf[la]) + list(rc_o[la].values()):
            cp.wait_send()

    def normed(wide):
        return (wide * lax.rsqrt(jnp.mean(wide * wide, axis=-1, keepdims=True) + NORM_EPS)).astype(BF16)

    def row_loop(count, fn):
        def body(i, _):
            fn(pl.ds(pl.multiple_of(i * NORM_ROWS, NORM_ROWS), NORM_ROWS))
            return 0

        lax.fori_loop(0, count // NORM_ROWS, body, 0)

    cp_x.start()
    cp_cos.start()
    cp_sin.start()
    cp_ks[0].start()
    cp_vs[0].start()
    for hp in range(PAIRS):
        cp_wq[0][hp].start()
    cp_wk[0].start()
    cp_wv[0].start()
    pl.semaphore_wait(barrier, 3)
    rc_x.start()
    prep_cache(0)
    cp_cos.wait()
    cp_sin.wait()
    cp_x.wait()
    rc_x.wait_recv()
    project(0, xbuf)
    for hp in range(PAIRS):
        cp_wq[1][hp].start()
    cp_wk[1].start()
    cp_wv[1].start()
    cp_wo[0].start()
    for slot in range(ff_slots):
        for cp in ff_copies(slot, slot, ff_chunk):
            cp.start()
    attention(0)
    prep_cache(1)
    finish_attention(0)
    for n in range(ncol):
        rc_y1[n].wait()

    def first_norm(rs):
        parts = [(ysend[n, rs, :] + yrecv[n, rs, :]).astype(BF16).astype(F32) for n in range(ncol)]
        res = (xbuf[rs, :].astype(F32) + jnp.concatenate(parts, axis=1)).astype(BF16)
        hbuf[rs, :] = res
        ubuf[rs, :] = normed(res.astype(F32))

    row_loop(ctok, first_norm)
    cp_wo[1].start()

    def gate_up(slot, size):
        gate = jnp.dot(ubuf[...], w1s[slot, :, pl.ds(0, size)], preferred_element_type=F32).astype(BF16).astype(F32)
        up = jnp.dot(ubuf[...], w3s[slot, :, pl.ds(0, size)], preferred_element_type=F32).astype(BF16).astype(F32)
        return (jax.nn.silu(gate) * up).astype(BF16)

    def down(slot, size):
        for n in range(ncol):
            macc[n] += jnp.dot(ebuf[:, pl.ds(0, size)], w2s[slot, pl.ds(0, size), pl.ds(n * cw, cw)], preferred_element_type=F32)

    def refill(chunk, which):
        for size, cond in ((ff_chunk, chunk < nfull), (tail, chunk == nfull)):
            if size:
                @pl.when(cond)
                def _(size=size):
                    cps = ff_copies(chunk, lax.rem(chunk, ff_slots), size)
                    for w in which:
                        cps[w].start()

    macc[...] = jnp.zeros(macc.shape, F32)
    first = ff_copies(0, 0, ff_chunk)
    first[0].wait()
    first[1].wait()
    ebuf[...] = gate_up(0, ff_chunk)
    refill(jnp.int32(ff_slots), (0, 1))

    def mlp_body(k, _):
        slot, prev = lax.rem(k, ff_slots), lax.rem(k - 1, ff_slots)
        cps = ff_copies(k, slot, ff_chunk)
        cps[0].wait()
        cps[1].wait()
        ff_copies(k - 1, prev, ff_chunk)[2].wait()
        hidden = gate_up(slot, ff_chunk)
        down(prev, ff_chunk)
        ebuf[...] = hidden
        refill(k + ff_slots, (0, 1))
        refill(k - 1 + ff_slots, (2,))
        return 0

    lax.fori_loop(1, nfull, mlp_body, 0)
    last_slot = (nfull - 1) % ff_slots
    ff_copies(nfull - 1, last_slot, ff_chunk)[2].wait()
    if tail:
        slot = nfull % ff_slots
        cps = ff_copies(nfull, slot, tail)
        cps[0].wait()
        cps[1].wait()
        hidden = gate_up(slot, tail)
        down(last_slot, ff_chunk)
        ebuf[:, pl.ds(0, tail)] = hidden
        cps[2].wait()
        down(slot, tail)
    else:
        down(last_slot, ff_chunk)
    for n in range(ncol):
        rc_m[n].start()
    for n in range(ncol):
        rc_m[n].wait()

    def second_norm(rs):
        acc = jnp.concatenate([macc[n, rs, :] + mrecv[n, rs, :] for n in range(ncol)], axis=1)
        res = (hbuf[rs, :].astype(F32) + acc).astype(BF16)
        hbuf[rs, :] = res
        ubuf[rs, :] = normed(res.astype(F32))

    row_loop(ctok, second_norm)
    gout[0] = hbuf[my_rows, :]
    cp_g.start()

    project(1, ubuf)
    attention(1)
    finish_attention(1)
    for n in range(ncol):
        rc_y2[n].wait()
        gout[1, :, pl.ds(n * cw, cw)] = (ysend[n, my_rows, :] + mrecv[n, pl.ds(ctok, tok), :]).astype(BF16)
    cp_y.start()
    rc_x.wait_send()
    rc_k[1].wait_send()
    rc_v[1].wait_send()
    for cp in cp_kout + cp_vout + [cp_g, cp_y]:
        cp.wait()


def solution(mesh):
    axis_size = mesh.shape["cp"]
    nchip = axis_size // 2
    ff_chunk, ff_slots = 512, 3
    rows_spec = P(("dp", "cp"), None)
    cache_spec = P(("dp", "cp"), None, None)
    mat_spec = P(None, None)
    vec_spec = P(None)
    layer_specs = (cache_spec, cache_spec, mat_spec, vec_spec, mat_spec, vec_spec, mat_spec, mat_spec)
    in_specs = (rows_spec,) + layer_specs + (mat_spec, mat_spec, mat_spec) + layer_specs
    out_specs = (rows_spec, rows_spec, cache_spec, cache_spec, cache_spec, cache_spec)

    def forward(x_in, cache_k1, cache_v1, w_q1, b_q1, w_k1, b_k1, w_v1, w_o1, w_gate, w_up, w_down,
                cache_k2, cache_v2, w_q2, b_q2, w_k2, b_k2, w_v2, w_o2):
        tok, width = x_in.shape
        cache_dev, kv_heads, hd = cache_k1.shape
        ctok = 2 * tok
        rows = 2 * ctok
        keys_tot = 2 * cache_dev + ctok
        cos_t, sin_t = rope_tables(axis_size * cache_dev, axis_size * tok, hd)
        bias = jnp.concatenate([b_q1, b_k1, b_q2, b_k2]).astype(F32).reshape(-1, hd)
        flat = lambda arr: arr.reshape(-1, hd)
        half_w = width // 2
        ncol = 4
        hbm = pl.BlockSpec(memory_space=pl.ANY)
        vmem = pl.BlockSpec(memory_space=pltpu.VMEM)
        scratch = [
            pltpu.VMEM((ctok, width), BF16),
            pltpu.VMEM((ctok, width), BF16),
            pltpu.VMEM((ctok, width), BF16),
            pltpu.VMEM((PAIRS, width, rows), BF16),
            pltpu.VMEM(w_k1.shape, BF16),
            pltpu.VMEM(w_v1.shape, BF16),
            pltpu.VMEM((half_w, width), BF16),
            pltpu.VMEM((2, keys_tot, hd), BF16),
            pltpu.VMEM((2, hd, keys_tot), BF16),
            pltpu.VMEM((2 * cache_dev, hd), BF16),
            pltpu.VMEM((2 * cache_dev, hd), BF16),
            pltpu.VMEM((cache_dev, hd), BF16),
            pltpu.VMEM((hd, cache_dev), BF16),
            pltpu.VMEM((2 * hd, hd), F32),
            pltpu.VMEM((2, UNITS, rows, hd), BF16),
            pltpu.VMEM((keys_tot, rows), F32),
            pltpu.VMEM((keys_tot, rows), F32),
            pltpu.VMEM((8, rows), F32),
            pltpu.VMEM((8, rows), F32),
            pltpu.VMEM((UNITS, hd + 8, rows), F32),
            pltpu.VMEM((2, PAIRS, hd + 8, rows), F32),
            pltpu.VMEM((2, 2, PAIRS, hd + 8, rows), F32),
            pltpu.VMEM((ctok, half_w), BF16),
            pltpu.VMEM((ncol, ctok, width // ncol), F32),
            pltpu.VMEM((ncol, ctok, width // ncol), F32),
            pltpu.VMEM((ncol, ctok, width // ncol), F32),
            pltpu.VMEM((ncol, ctok + tok, width // ncol), F32),
            pltpu.VMEM((ff_slots, width, ff_chunk), BF16),
            pltpu.VMEM((ff_slots, width, ff_chunk), BF16),
            pltpu.VMEM((ff_slots, ff_chunk, width), BF16),
            pltpu.VMEM((ctok, ff_chunk), BF16),
            pltpu.VMEM((ctok, hd), F32),
            pltpu.VMEM((ctok, hd), F32),
            pltpu.VMEM((2, 2, 2 * tok, hd), BF16),
            pltpu.VMEM((2, tok, width), BF16),
            pltpu.SemaphoreType.DMA((29,)),
            pltpu.SemaphoreType.DMA((3, ff_slots)),
            pltpu.SemaphoreType.DMA((65,)),
            pltpu.SemaphoreType.DMA((65,)),
        ]
        act = jax.ShapeDtypeStruct((tok, width), BF16)
        app = jax.ShapeDtypeStruct((kv_heads * tok, hd), BF16)
        outs = pl.pallas_call(
            functools.partial(block_kernel, nchip, ff_chunk, ff_slots),
            out_shape=(act, act, app, app, app, app),
            in_specs=[hbm] * 16 + [vmem, hbm, hbm],
            out_specs=(hbm,) * 6,
            scratch_shapes=scratch,
            compiler_params=pltpu.CompilerParams(collective_id=0, has_side_effects=True, vmem_limit_bytes=67043328),
        )(x_in, flat(cache_k1), flat(cache_v1), w_q1, w_k1, w_v1, w_o1, w_gate, w_up, w_down,
          flat(cache_k2), flat(cache_v2), w_q2, w_k2, w_v2, w_o2, bias, jnp.asarray(cos_t), jnp.asarray(sin_t))
        hidden, y_two = outs[:2]
        appends = [arr.reshape(tok, kv_heads, hd) for arr in outs[2:]]
        return (hidden, y_two, *appends)

    return jax.shard_map(forward, mesh=mesh, in_specs=in_specs, out_specs=out_specs, check_vma=False)
```

```python
import functools
import math

import jax
import jax.numpy as jnp
import numpy as np
from jax import lax
from jax.experimental import pallas as pl
from jax.experimental.pallas import tpu as pltpu
from jax.sharding import PartitionSpec as P

ROPE_THETA = 500000.0
NORM_EPS = 1e-5
MESH = pl.DeviceIdType.MESH
scope = jax.named_scope
F32 = jnp.float32
BF16 = jnp.bfloat16

ORDER = ("own0", "own1", "own2", "left0", "right1", "opp0", "opp1", "left2", "right3", "opp2", "opp3",
         "right0", "left1", "right2", "left3", "own3")
SLOT = {name: idx for idx, name in enumerate(ORDER)}
UNITS = len(ORDER)
PAIRS = 4
NORM_ROWS = 16


def rope_tables(first_pos, count, head_dim):
    half_dim = head_dim // 2
    exponent = np.arange(half_dim, dtype=np.float32) * np.float32(2.0 / head_dim)
    inv_freq = (np.float32(1.0) / np.power(np.float32(ROPE_THETA), exponent)).astype(np.float32)
    positions = (first_pos + np.arange(count)).astype(np.float32)
    angles = (positions[:, None] * inv_freq[None, :]).astype(np.float32)
    cos_t = np.cos(angles.astype(np.float64)).astype(np.float32)
    sin_t = np.sin(angles.astype(np.float64)).astype(np.float32)
    return np.concatenate([cos_t, cos_t], axis=1), np.concatenate([-sin_t, sin_t], axis=1)


def block_kernel(nchip, ff_chunk, ff_slots,
                 x_hbm, kc1, vc1, wq1, wk1, wv1, wo1, w_gate, w_up, w_down, kc2, vc2, wq2, wk2, wv2, wo2,
                 bq1, bk1, bq2, bk2, cos_hbm, sin_hbm,
                 g_out, y_out, k1_out, v1_out, k2_out, v2_out,
                 xbuf, hbuf, ubuf, wkb, wvb, wob, kall, vtall, kstage, vstage, ksend, vsend, deint,
                 qall, s_a, s_b, m_a, m_b, obuf, relay, final, ohalf, ysend, yrecv, mrecv,
                 w1s, w3s, w2s, ebuf, cosb, sinb, bqb, bkb, kvout, gout,
                 dsem, rings, ssem, rsem):
    tok = x_hbm.shape[0]
    ctok = 2 * tok
    width = x_hbm.shape[1]
    hd = kc1.shape[1]
    keys_dev = kc1.shape[0] // 2
    keys_chip = 2 * keys_dev
    keys_tot = keys_chip + ctok
    rows = 2 * ctok
    half_w = width // 2
    ncol = 4
    cw = width // ncol
    cexp = math.log2(math.e) / math.sqrt(hd)

    me = lax.axis_index("cp")
    chip = me // 2
    core = lax.rem(me, 2)
    partner = chip * 2 + 1 - core
    left_chip = lax.rem(chip + nchip - 1, nchip)
    right_chip = lax.rem(chip + 1, nchip)
    opp_chip = lax.rem(chip + 2, nchip)
    left = left_chip * 2 + core
    right = right_chip * 2 + core

    macc = ysend
    dcount = [0]

    def local(src, dst):
        idx = dcount[0]
        dcount[0] += 1
        return pltpu.make_async_copy(src, dst, dsem.at[idx])

    rcount = [0]

    def remote(src, dst, dev):
        idx = rcount[0]
        rcount[0] += 1
        return pltpu.make_async_remote_copy(src_ref=src, dst_ref=dst, send_sem=ssem.at[idx], recv_sem=rsem.at[idx],
                                            device_id={"cp": dev}, device_id_type=MESH)

    barrier = pltpu.get_barrier_semaphore()
    for dev in (partner, left, right):
        pl.semaphore_signal(barrier, inc=1, device_id={"cp": dev}, device_id_type=MESH)

    my_rows = pl.ds(pl.multiple_of(core * tok, tok), tok)
    kc = (kc1, kc2)
    vc = (vc1, vc2)
    wq = (wq1, wq2)
    wk = (wk1, wk2)
    wv = (wv1, wv2)
    wo = (wo1, wo2)
    k_out = (k1_out, k2_out)
    v_out = (v1_out, v2_out)

    cp_x = local(x_hbm, xbuf.at[my_rows])
    pos_rows = pl.ds(pl.multiple_of(chip * ctok, ctok), ctok)
    cp_cos = local(cos_hbm.at[pos_rows], cosb)
    cp_sin = local(sin_hbm.at[pos_rows], sinb)
    cp_bq = [local(ref, bqb.at[la]) for la, ref in enumerate((bq1, bq2))]
    cp_bk = [local(ref, bkb.at[la]) for la, ref in enumerate((bk1, bk2))]
    cp_ks = [local(kc[la], kstage) for la in range(2)]
    cp_vs = [local(vc[la], vstage) for la in range(2)]
    qcol = [pl.ds(pl.multiple_of(core * half_w + hp * rows, rows), rows) for hp in range(PAIRS)]
    wqb = [(w1s, w3s)[hp // 2].at[ff_slots - 1, :, pl.ds((hp % 2) * rows, rows)] for hp in range(PAIRS)]
    cp_wq = [[local(wq[la].at[:, qcol[hp]], wqb[hp]) for hp in range(PAIRS)] for la in range(2)]
    cp_wk = [local(wk[la], wkb) for la in range(2)]
    cp_wv = [local(wv[la], wvb) for la in range(2)]
    cp_wo = [local(wo[la].at[pl.ds(pl.multiple_of(core * half_w, half_w), half_w)], wob) for la in range(2)]
    cp_kout = [local(kvout.at[la, 0], k_out[la]) for la in range(2)]
    cp_vout = [local(kvout.at[la, 1], v_out[la]) for la in range(2)]
    cp_g = local(gout.at[0], g_out)
    cp_y = local(gout.at[1], y_out)

    rc_x = remote(x_hbm, xbuf.at[my_rows], partner)
    rc_k = [remote(ksend, kall.at[la, pl.ds(keys_dev, keys_dev)], partner) for la in range(2)]
    rc_v = [remote(vsend, vtall.at[la, :, pl.ds(keys_dev, keys_dev)], partner) for la in range(2)]
    rc_qr, rc_ql, rc_qf, rc_o = [], [], [], []
    for la in range(2):
        own = [qall.at[SLOT["own%d" % hp]] for hp in range(PAIRS)]
        rc_qr.append([remote(own[hp], qall.at[SLOT["left%d" % hp]], right) for hp in range(PAIRS)])
        rc_ql.append([remote(own[hp], qall.at[SLOT["right%d" % hp]], left) for hp in range(PAIRS)])
        fwd = []
        for hp in range(PAIRS):
            side, dev = ("left", right) if hp % 2 == 0 else ("right", left)
            fwd.append(remote(qall.at[SLOT["%s%d" % (side, hp)]], qall.at[SLOT["opp%d" % hp]], dev))
        rc_qf.append(fwd)
        outs = {}
        for hp in range(PAIRS):
            outs["left%d" % hp] = remote(obuf.at[SLOT["left%d" % hp]], final.at[1, hp], left)
            outs["right%d" % hp] = remote(obuf.at[SLOT["right%d" % hp]], final.at[0, hp], right)
            outs["opp%d" % hp] = remote(obuf.at[SLOT["opp%d" % hp]], relay.at[hp], right if hp % 2 == 0 else left)
        rc_o.append(outs)
    rc_y1 = [remote(ysend.at[n], yrecv.at[n], partner) for n in range(ncol)]
    other_rows = pl.ds(pl.multiple_of((1 - core) * tok, tok), tok)
    rc_y2 = [remote(ysend.at[n, other_rows], yrecv.at[n, pl.ds(0, tok)], partner) for n in range(ncol)]
    rc_m = [remote(macc.at[n], mrecv.at[n], partner) for n in range(ncol)]

    ff_half = w_gate.shape[1] // 2
    nfull = ff_half // ff_chunk
    tail = ff_half - nfull * ff_chunk

    def ff_copies(chunk, slot, size):
        cols = pl.ds(pl.multiple_of(core * ff_half + chunk * ff_chunk, 128), size)
        return (pltpu.make_async_copy(w_gate.at[:, cols], w1s.at[slot, :, pl.ds(0, size)], rings.at[0, slot]),
                pltpu.make_async_copy(w_up.at[:, cols], w3s.at[slot, :, pl.ds(0, size)], rings.at[1, slot]),
                pltpu.make_async_copy(w_down.at[cols], w2s.at[slot, pl.ds(0, size)], rings.at[2, slot]))

    def rope(val, la_bias, cos_v, sin_v):
        val = (val + la_bias).astype(BF16).astype(F32)
        return (val * cos_v + pltpu.roll(val, hd // 2, 1) * sin_v).astype(BF16)

    def prep_cache(la):
        if la == 1:
            rc_k[0].wait_send()
            rc_v[0].wait_send()
        step_rows = 2 * hd

        def split(ref, i):
            deint[...] = ref[pl.ds(pl.multiple_of(i * step_rows, step_rows), step_rows), :].astype(F32)
            head0 = deint[pl.ds(0, hd, stride=2), :]
            head1 = deint[pl.ds(1, hd, stride=2), :]
            is0 = core == 0
            return jnp.where(is0, head0, head1), jnp.where(is0, head1, head0)

        def kbody(i, _):
            mine, other = split(kstage, i)
            at = pl.ds(pl.multiple_of(i * hd, hd), hd)
            kall[la, at, :] = mine.astype(BF16)
            ksend[at, :] = other.astype(BF16)
            return 0

        def vbody(i, _):
            mine, other = split(vstage, i)
            at = pl.ds(pl.multiple_of(i * hd, hd), hd)
            vtall[la, :, at] = mine.T.astype(BF16)
            vsend[:, at] = other.T.astype(BF16)
            return 0

        cp_ks[la].wait()
        lax.fori_loop(0, keys_dev // hd, kbody, 0)
        rc_k[la].start()
        cp_vs[la].wait()
        lax.fori_loop(0, keys_dev // hd, vbody, 0)
        rc_v[la].start()
        if la == 0:
            cp_ks[1].start()
            cp_vs[1].start()

    def project(la, in_ref):
        heads_half = half_w // hd
        bq_v = bqb[la].astype(F32)
        bq_v = jnp.where(core == 0, bq_v[:heads_half], bq_v[heads_half:])
        bk_v = bkb[la].astype(F32)
        cos_v, sin_v = cosb[...], sinb[...]
        for hp in range(PAIRS):
            cp_wq[la][hp].wait()
            acc = jnp.dot(in_ref[...], wqb[hp][...], preferred_element_type=F32)
            slot = SLOT["own%d" % hp]
            for j in range(2):
                row = hp * 2 + j
                qall[slot, pl.ds(j * ctok, ctok), :] = rope(acc[:, j * hd:(j + 1) * hd], bq_v[row:row + 1], cos_v, sin_v)
            rc_qr[la][hp].start()
            rc_ql[la][hp].start()
        cp_wk[la].wait()
        acc = jnp.dot(in_ref[...], wkb[...], preferred_element_type=F32)
        k_heads = [rope(acc[:, j * hd:(j + 1) * hd], bk_v[j:j + 1], cos_v, sin_v).astype(F32) for j in range(2)]
        cp_wv[la].wait()
        acc = jnp.dot(in_ref[...], wvb[...], preferred_element_type=F32)
        v_heads = [acc[:, j * hd:(j + 1) * hd].astype(BF16).astype(F32) for j in range(2)]
        is0 = core == 0
        kall[la, pl.ds(keys_chip, ctok), :] = jnp.where(is0, k_heads[0], k_heads[1]).astype(BF16)
        vtall[la, :, pl.ds(keys_chip, ctok)] = jnp.where(is0, v_heads[0], v_heads[1]).T.astype(BF16)
        for which, heads in ((0, k_heads), (1, v_heads)):
            for j in range(2):
                mine = jnp.where(is0, heads[j][:tok], heads[j][tok:])
                deint[pl.ds(j, tok, stride=2), :] = mine
            kvout[la, which] = deint[pl.ds(0, 2 * tok), :].astype(BF16)
        cp_kout[la].start()
        cp_vout[la].start()

    offs = {"own": 0, "left": (left_chip - chip) * ctok, "right": (right_chip - chip) * ctok, "opp": (opp_chip - chip) * ctok}

    def unit_offset(unit):
        res = jnp.int32(0)
        for name, idx in SLOT.items():
            if not name.startswith("own"):
                res = jnp.where(unit == idx, offs[name[:-1]], res)
        return res

    def scores(la, unit, s_ref, m_ref):
        s_val = lax.dot_general(kall[la], qall[unit], (((1,), (1,)), ((), ())), preferred_element_type=F32)
        s_ref[pl.ds(0, keys_chip), :] = s_val[:keys_chip]
        peak = jnp.max(s_val[:keys_chip].reshape(keys_chip // 8, 8, rows), axis=0)
        key_i = lax.broadcasted_iota(jnp.int32, (ctok, rows), 0)
        tok_i = lax.broadcasted_iota(jnp.int32, (ctok, rows), 1) % ctok
        masked = jnp.where(key_i - tok_i <= unit_offset(unit), s_val[keys_chip:], -jnp.inf)
        s_ref[pl.ds(keys_chip, ctok), :] = masked
        m_ref[...] = jnp.maximum(peak, jnp.max(masked.reshape(ctok // 8, 8, rows), axis=0))

    row8 = lax.broadcasted_iota(jnp.int32, (8, rows), 0)

    def put(dst, out_v, peak, total):
        dst[pl.ds(0, hd), :] = out_v
        dst[pl.ds(hd, 8), :] = jnp.where(row8 == 0, peak, total)

    def get(src):
        return src[pl.ds(0, hd), :], src[pl.ds(hd, 1), :], src[pl.ds(hd + 1, 1), :]

    def merged(parts):
        peak = functools.reduce(jnp.maximum, [part[1] for part in parts])
        scales = [jnp.exp2((part[1] - peak) * cexp) for part in parts]
        out_v = functools.reduce(jnp.add, [part[0] * sc for part, sc in zip(parts, scales)])
        total = functools.reduce(jnp.add, [part[2] * sc for part, sc in zip(parts, scales)])
        return out_v, peak, total

    def attend_unit(la, unit, nxt, s_cur, m_cur, s_nxt, m_nxt):
        peak = jnp.max(m_cur[...], axis=0, keepdims=True)
        shift = jnp.broadcast_to(peak * cexp, (8, rows))
        prob = jnp.exp2(s_cur[...].reshape(keys_tot // 8, 8, rows) * cexp - shift[None])
        total = jnp.sum(jnp.sum(prob, axis=0), axis=0, keepdims=True)
        out_v = jnp.dot(vtall[la], prob.reshape(keys_tot, rows).astype(BF16), preferred_element_type=F32)
        scores(la, nxt, s_nxt, m_nxt)
        put(obuf.at[unit], out_v, peak, total)

    def before(la):
        acts = {}

        def add(name, *fns):
            acts.setdefault(SLOT[name] - 1, []).extend(fns)

        for hp in range(PAIRS):
            lw, rw = rc_qr[la][hp].wait_recv, rc_ql[la][hp].wait_recv
            fwd = rc_qf[la][hp]
            if hp % 2 == 0:
                acts.setdefault(2 if hp == 0 else 4, []).extend([lw, fwd.start])
                add("right%d" % hp, rw)
            else:
                acts.setdefault(3 if hp == 1 else 5, []).extend([rw, fwd.start])
                add("left%d" % hp, lw)
        for hp in range(PAIRS):
            add("opp%d" % hp, rc_qf[la][hp].wait_recv)
        return acts

    def after(la):
        acts = {}
        for name, cp in rc_o[la].items():
            hp = int(name[-1])
            merge_it = (name.startswith("right") and hp % 2 == 0) or (name.startswith("left") and hp % 2 == 1)

            def act(name=name, cp=cp, hp=hp, merge_it=merge_it):
                if name.startswith("left" if hp % 2 == 0 else "right"):
                    rc_qf[la][hp].wait_send()
                if merge_it:
                    rc_o[la]["opp%d" % hp].wait_recv()
                    put(obuf.at[SLOT[name]], *merged([get(obuf.at[SLOT[name]]), get(relay.at[hp])]))
                cp.start()

            acts[SLOT[name]] = [act]
        return acts

    def attention(la):
        rc_k[la].wait_recv()
        rc_v[la].wait_recv()
        with scope("score0"):
            scores(la, 0, s_a, m_a)
        pre, post = before(la), after(la)

        def run(acts, pair, parity):
            for unit, fns in acts.items():
                if unit % 2 == parity:
                    @pl.when(pair == unit // 2)
                    def _(fns=fns):
                        with scope("event"):
                            for fn in fns:
                                fn()

        def body(pair, _):
            run(pre, pair, 0)
            attend_unit(la, 2 * pair, 2 * pair + 1, s_a, m_a, s_b, m_b)
            run(post, pair, 0)
            run(pre, pair, 1)
            attend_unit(la, 2 * pair + 1, jnp.minimum(2 * pair + 2, UNITS - 1), s_b, m_b, s_a, m_a)
            run(post, pair, 1)
            return 0

        lax.fori_loop(0, UNITS // 2, body, 0)

    def finish_attention(la):
        for hp in range(PAIRS):
            with scope("owait"):
                rc_o[la]["right%d" % hp].wait_recv()
                rc_o[la]["left%d" % hp].wait_recv()
            out_v, _, total = merged([get(obuf.at[SLOT["own%d" % hp]]), get(final.at[0, hp]), get(final.at[1, hp])])
            out_v = out_v / total
            for j in range(2):
                ohalf[:, pl.ds((2 * hp + j) * hd, hd)] = out_v[:, j * ctok:(j + 1) * ctok].T.astype(BF16)
        cp_wo[la].wait()
        rc_y = (rc_y1, rc_y2)[la]
        for n in range(ncol):
            ysend[n] = jnp.dot(ohalf[...], wob[:, n * cw:(n + 1) * cw], preferred_element_type=F32)
            rc_y[n].start()
        for cp in list(rc_qr[la]) + list(rc_ql[la]) + list(rc_o[la].values()):
            cp.wait_send()

    def normed(wide):
        return (wide * lax.rsqrt(jnp.mean(wide * wide, axis=-1, keepdims=True) + NORM_EPS)).astype(BF16)

    def row_loop(count, fn):
        def body(i, _):
            fn(pl.ds(pl.multiple_of(i * NORM_ROWS, NORM_ROWS), NORM_ROWS))
            return 0

        lax.fori_loop(0, count // NORM_ROWS, body, 0)

    cp_x.start()
    cp_cos.start()
    cp_sin.start()
    for cp in cp_bq + cp_bk:
        cp.start()
    cp_ks[0].start()
    cp_vs[0].start()
    for hp in range(PAIRS):
        cp_wq[0][hp].start()
    cp_wk[0].start()
    cp_wv[0].start()
    with scope("entry"):
        pl.semaphore_wait(barrier, 3)
    rc_x.start()
    with scope("prep0"):
        prep_cache(0)
    cp_cos.wait()
    cp_sin.wait()
    for cp in cp_bq + cp_bk:
        cp.wait()
    cp_x.wait()
    with scope("xwait"):
        rc_x.wait_recv()
    with scope("proj0"):
        project(0, xbuf)
    cp_wo[0].start()
    cp_wk[1].start()
    cp_wv[1].start()
    for slot in range(ff_slots):
        for cp in ff_copies(slot, slot, ff_chunk):
            cp.start()
    with scope("attn0"):
        attention(0)
    with scope("prep1"):
        prep_cache(1)
    with scope("fin0"):
        finish_attention(0)
    with scope("ywait"):
        for n in range(ncol):
            rc_y1[n].wait()

    def first_norm(rs):
        parts = [(ysend[n, rs, :] + yrecv[n, rs, :]).astype(BF16).astype(F32) for n in range(ncol)]
        res = (xbuf[rs, :].astype(F32) + jnp.concatenate(parts, axis=1)).astype(BF16)
        hbuf[rs, :] = res
        ubuf[rs, :] = normed(res.astype(F32))

    with scope("norm1"):
        row_loop(ctok, first_norm)

    def gate_up(slot, size):
        gate = jnp.dot(ubuf[...], w1s[slot, :, pl.ds(0, size)], preferred_element_type=F32).astype(BF16).astype(F32)
        up = jnp.dot(ubuf[...], w3s[slot, :, pl.ds(0, size)], preferred_element_type=F32).astype(BF16).astype(F32)
        return (jax.nn.silu(gate) * up).astype(BF16)

    def down(slot, size, send=False):
        for n in range(ncol):
            macc[n] += jnp.dot(ebuf[:, pl.ds(0, size)], w2s[slot, pl.ds(0, size), pl.ds(n * cw, cw)], preferred_element_type=F32)
            if send:
                rc_m[n].start()

    def refill(chunk, which):
        for size, cond in ((ff_chunk, chunk < nfull), (tail, chunk == nfull)):
            if size:
                @pl.when(cond)
                def _(size=size):
                    cps = ff_copies(chunk, lax.rem(chunk, ff_slots), size)
                    for w in which:
                        cps[w].start()

    macc[...] = jnp.zeros(macc.shape, F32)
    first = ff_copies(0, 0, ff_chunk)
    first[0].wait()
    first[1].wait()
    ebuf[...] = gate_up(0, ff_chunk)
    refill(jnp.int32(ff_slots), (0, 1))

    def mlp_body(k, _):
        slot, prev = lax.rem(k, ff_slots), lax.rem(k - 1, ff_slots)
        cps = ff_copies(k, slot, ff_chunk)
        cps[0].wait()
        cps[1].wait()
        ff_copies(k - 1, prev, ff_chunk)[2].wait()
        hidden = gate_up(slot, ff_chunk)
        down(prev, ff_chunk)
        ebuf[...] = hidden
        refill(k + ff_slots, (0, 1))
        refill(k - 1 + ff_slots, (2,))
        return 0

    with scope("mlp"):
        lax.fori_loop(1, nfull, mlp_body, 0)
    for hp in range(PAIRS):
        cp_wq[1][hp].start()
    cp_wo[1].start()
    last_slot = (nfull - 1) % ff_slots
    ff_copies(nfull - 1, last_slot, ff_chunk)[2].wait()
    if tail:
        slot = nfull % ff_slots
        cps = ff_copies(nfull, slot, tail)
        cps[0].wait()
        cps[1].wait()
        hidden = gate_up(slot, tail)
        down(last_slot, ff_chunk)
        ebuf[:, pl.ds(0, tail)] = hidden
        cps[2].wait()
        down(slot, tail, send=True)
    else:
        down(last_slot, ff_chunk, send=True)
    with scope("mwait"):
        for n in range(ncol):
            rc_m[n].wait()

    def second_norm(rs):
        acc = jnp.concatenate([macc[n, rs, :] + mrecv[n, rs, :] for n in range(ncol)], axis=1)
        res = (hbuf[rs, :].astype(F32) + acc).astype(BF16)
        hbuf[rs, :] = res
        ubuf[rs, :] = normed(res.astype(F32))

    with scope("norm2"):
        row_loop(ctok, second_norm)
    gout[0] = hbuf[my_rows, :]
    cp_g.start()

    with scope("proj1"):
        project(1, ubuf)
    with scope("attn1"):
        attention(1)
    with scope("fin1"):
        finish_attention(1)
    for n in range(ncol):
        rc_y2[n].wait()
        gout[1, :, pl.ds(n * cw, cw)] = (ysend[n, my_rows, :] + yrecv[n, pl.ds(0, tok), :]).astype(BF16)
    cp_y.start()
    rc_x.wait_send()
    rc_k[1].wait_send()
    rc_v[1].wait_send()
    for cp in cp_kout + cp_vout + [cp_g, cp_y]:
        cp.wait()


def copy_out(*refs):
    half = len(refs) // 2
    for src, dst in zip(refs[:half], refs[half:]):
        dst[...] = src[...]


def solution(mesh):
    axis_size = mesh.shape["cp"]
    nchip = axis_size // 2
    ff_chunk, ff_slots = 512, 5
    rows_spec = P(("dp", "cp"), None)
    cache_spec = P(("dp", "cp"), None, None)
    mat_spec = P(None, None)
    vec_spec = P(None)
    layer_specs = (cache_spec, cache_spec, mat_spec, vec_spec, mat_spec, vec_spec, mat_spec, mat_spec)
    in_specs = (rows_spec,) + layer_specs + (mat_spec, mat_spec, mat_spec) + layer_specs
    out_specs = (rows_spec, rows_spec, cache_spec, cache_spec, cache_spec, cache_spec)

    def forward(x_in, cache_k1, cache_v1, w_q1, b_q1, w_k1, b_k1, w_v1, w_o1, w_gate, w_up, w_down,
                cache_k2, cache_v2, w_q2, b_q2, w_k2, b_k2, w_v2, w_o2):
        tok, width = x_in.shape
        cache_dev, kv_heads, hd = cache_k1.shape
        ctok = 2 * tok
        rows = 2 * ctok
        keys_tot = 2 * cache_dev + ctok
        cos_t, sin_t = rope_tables(axis_size * cache_dev, axis_size * tok, hd)
        flat = lambda arr: arr.reshape(-1, hd)
        half_w = width // 2
        ncol = 4
        hbm = pl.BlockSpec(memory_space=pl.ANY)
        scratch = [
            pltpu.VMEM((ctok, width), BF16),
            pltpu.VMEM((ctok, width), BF16),
            pltpu.VMEM((ctok, width), BF16),
            pltpu.VMEM(w_k1.shape, BF16),
            pltpu.VMEM(w_v1.shape, BF16),
            pltpu.VMEM((half_w, width), BF16),
            pltpu.VMEM((2, keys_tot, hd), BF16),
            pltpu.VMEM((2, hd, keys_tot), BF16),
            pltpu.VMEM((2 * cache_dev, hd), BF16),
            pltpu.VMEM((2 * cache_dev, hd), BF16),
            pltpu.VMEM((cache_dev, hd), BF16),
            pltpu.VMEM((hd, cache_dev), BF16),
            pltpu.VMEM((2 * hd, hd), F32),
            pltpu.VMEM((UNITS, rows, hd), BF16),
            pltpu.VMEM((keys_tot, rows), F32),
            pltpu.VMEM((keys_tot, rows), F32),
            pltpu.VMEM((8, rows), F32),
            pltpu.VMEM((8, rows), F32),
            pltpu.VMEM((UNITS, hd + 8, rows), F32),
            pltpu.VMEM((PAIRS, hd + 8, rows), F32),
            pltpu.VMEM((2, PAIRS, hd + 8, rows), F32),
            pltpu.VMEM((ctok, half_w), BF16),
            pltpu.VMEM((ncol, ctok, width // ncol), F32),
            pltpu.VMEM((ncol, ctok, width // ncol), F32),
            pltpu.VMEM((ncol, ctok, width // ncol), F32),
            pltpu.VMEM((ff_slots, width, ff_chunk), BF16),
            pltpu.VMEM((ff_slots, width, ff_chunk), BF16),
            pltpu.VMEM((ff_slots, ff_chunk, width), BF16),
            pltpu.VMEM((ctok, ff_chunk), BF16),
            pltpu.VMEM((ctok, hd), F32),
            pltpu.VMEM((ctok, hd), F32),
            pltpu.VMEM((2, width // hd, hd), BF16),
            pltpu.VMEM((2, kv_heads, hd), BF16),
            pltpu.VMEM((2, 2, 2 * tok, hd), BF16),
            pltpu.VMEM((2, tok, width), BF16),
            pltpu.SemaphoreType.DMA((33,)),
            pltpu.SemaphoreType.DMA((3, ff_slots)),
            pltpu.SemaphoreType.DMA((65,)),
            pltpu.SemaphoreType.DMA((65,)),
        ]
        act = jax.ShapeDtypeStruct((tok, width), BF16)
        app = jax.ShapeDtypeStruct((kv_heads * tok, hd), BF16)
        outs = pl.pallas_call(
            functools.partial(block_kernel, nchip, ff_chunk, ff_slots),
            out_shape=(act, act, app, app, app, app),
            in_specs=[hbm] * 22,
            out_specs=(hbm,) * 6,
            scratch_shapes=scratch,
            compiler_params=pltpu.CompilerParams(collective_id=0, has_side_effects=True, vmem_limit_bytes=67043328),
        )(x_in, flat(cache_k1), flat(cache_v1), w_q1, w_k1, w_v1, w_o1, w_gate, w_up, w_down,
          flat(cache_k2), flat(cache_v2), w_q2, w_k2, w_v2, w_o2,
          flat(b_q1), flat(b_k1), flat(b_q2), flat(b_k2), jnp.asarray(cos_t), jnp.asarray(sin_t))
        outs = pl.pallas_call(copy_out, out_shape=[jax.ShapeDtypeStruct(arr.shape, arr.dtype) for arr in outs])(*outs)
        hidden, y_two = outs[:2]
        appends = [arr.reshape(tok, kv_heads, hd) for arr in outs[2:]]
        return (hidden, y_two, *appends)

    return jax.shard_map(forward, mesh=mesh, in_specs=in_specs, out_specs=out_specs, check_vma=False)
```

```python
import functools
import math

import jax
import jax.numpy as jnp
import numpy as np
from jax import lax
from jax.experimental import pallas as pl
from jax.experimental.pallas import tpu as pltpu
from jax.sharding import PartitionSpec as P

ROPE_THETA = 500000.0
NORM_EPS = 1e-5
MESH = pl.DeviceIdType.MESH
scope = jax.named_scope
F32 = jnp.float32
BF16 = jnp.bfloat16

ORDER = ("own0", "left0", "right1", "left2", "opp0", "opp1", "right3", "opp2", "opp3",
         "right0", "left1", "own1", "right2", "left3", "own2", "own3")
FORWARD_BEFORE = (0, 1, 2, 3)
SLOT = {name: idx for idx, name in enumerate(ORDER)}
UNITS = len(ORDER)
PAIRS = 4
NORM_ROWS = 32


def rope_tables(first_pos, count, head_dim):
    half_dim = head_dim // 2
    exponent = np.arange(half_dim, dtype=np.float32) * np.float32(2.0 / head_dim)
    inv_freq = (np.float32(1.0) / np.power(np.float32(ROPE_THETA), exponent)).astype(np.float32)
    positions = (first_pos + np.arange(count)).astype(np.float32)
    angles = (positions[:, None] * inv_freq[None, :]).astype(np.float32)
    cos_t = np.cos(angles.astype(np.float64)).astype(np.float32)
    sin_t = np.sin(angles.astype(np.float64)).astype(np.float32)
    return np.concatenate([cos_t, cos_t], axis=1), np.concatenate([-sin_t, sin_t], axis=1)


def block_kernel(nchip, ff_first, ff_chunk, ff_slots,
                 x_hbm, kc1, vc1, wq1, wk1, wv1, wo1, w_gate, w_up, w_down, kc2, vc2, wq2, wk2, wv2, wo2,
                 bq1, bk1, bq2, bk2, cos_hbm, sin_hbm,
                 g_out, y_out, k1_out, v1_out, k2_out, v2_out,
                 xbuf, hbuf, ubuf, wkvb, wob, kall, vtall, kstage, vstage, ksend, vsend, deint,
                 qall, m_a, m_b, obuf, relay, final, ohalf, ysend, yrecv, mrecv,
                 w1s, w3s, w2s, ebuf, cosb, sinb, bqb, bkb, kvout, gout,
                 dsem, rings, ssem, rsem):
    tok = x_hbm.shape[0]
    ctok = 2 * tok
    width = x_hbm.shape[1]
    hd = kc1.shape[1]
    keys_dev = kc1.shape[0] // 2
    keys_chip = 2 * keys_dev
    keys_tot = keys_chip + ctok
    rows = 2 * ctok
    half_w = width // 2
    ncol = 4
    cw = width // ncol
    cexp = math.log2(math.e) / math.sqrt(hd)

    me = lax.axis_index("cp")
    chip = me // 2
    core = lax.rem(me, 2)
    partner = chip * 2 + 1 - core
    left_chip = lax.rem(chip + nchip - 1, nchip)
    right_chip = lax.rem(chip + 1, nchip)
    opp_chip = lax.rem(chip + 2, nchip)
    left = left_chip * 2 + core
    right = right_chip * 2 + core

    macc = ysend
    dcount = [0]

    def local(src, dst):
        idx = dcount[0]
        dcount[0] += 1
        return pltpu.make_async_copy(src, dst, dsem.at[idx])

    rcount = [0]

    def remote(src, dst, dev):
        idx = rcount[0]
        rcount[0] += 1
        return pltpu.make_async_remote_copy(src_ref=src, dst_ref=dst, send_sem=ssem.at[idx], recv_sem=rsem.at[idx],
                                            device_id={"cp": dev}, device_id_type=MESH)

    barrier = pltpu.get_barrier_semaphore()
    for dev in (partner, left, right):
        pl.semaphore_signal(barrier, inc=1, device_id={"cp": dev}, device_id_type=MESH)

    my_rows = pl.ds(pl.multiple_of(core * tok, tok), tok)
    kc = (kc1, kc2)
    vc = (vc1, vc2)
    wq = (wq1, wq2)
    wk = (wk1, wk2)
    wv = (wv1, wv2)
    wo = (wo1, wo2)
    k_out = (k1_out, k2_out)
    v_out = (v1_out, v2_out)

    cp_x = local(x_hbm, xbuf.at[my_rows])
    pos_rows = pl.ds(pl.multiple_of(chip * ctok, ctok), ctok)
    cp_cos = local(cos_hbm.at[pos_rows], cosb)
    cp_sin = local(sin_hbm.at[pos_rows], sinb)
    cp_bq = [local(ref, bqb.at[la]) for la, ref in enumerate((bq1, bq2))]
    cp_bk = [local(ref, bkb.at[la]) for la, ref in enumerate((bk1, bk2))]
    cp_ks = [local(kc[la], kstage) for la in range(2)]
    cp_vs = [local(vc[la], vstage) for la in range(2)]
    qcol = [pl.ds(pl.multiple_of(core * half_w + half * 2 * rows, rows), 2 * rows) for half in range(2)]
    wqb = [ref.at[ff_slots - 1, :, pl.ds(0, 2 * rows)] for ref in (w1s, w3s)]
    cp_wq = [[local(wq[la].at[:, qcol[half]], wqb[half]) for half in range(2)] for la in range(2)]
    cp_wk = [local(wk[la], wkvb.at[:, pl.ds(0, 2 * hd)]) for la in range(2)]
    cp_wv = [local(wv[la], wkvb.at[:, pl.ds(2 * hd, 2 * hd)]) for la in range(2)]
    cp_wo = [local(wo[la].at[pl.ds(pl.multiple_of(core * half_w, half_w), half_w)], wob) for la in range(2)]
    cp_kout = [local(kvout.at[la, 0], k_out[la]) for la in range(2)]
    cp_vout = [local(kvout.at[la, 1], v_out[la]) for la in range(2)]
    cp_g = local(gout.at[0], g_out)
    cp_y = local(gout.at[1], y_out)

    rc_x = remote(x_hbm, xbuf.at[my_rows], partner)
    rc_k = [remote(ksend, kall.at[la, pl.ds(keys_dev, keys_dev)], partner) for la in range(2)]
    rc_v = [remote(vsend, vtall.at[la, :, pl.ds(keys_dev, keys_dev)], partner) for la in range(2)]
    rc_qr, rc_ql, rc_qf, rc_o = [], [], [], []
    for la in range(2):
        own = [qall.at[SLOT["own%d" % hp]] for hp in range(PAIRS)]
        rc_qr.append([remote(own[hp], qall.at[SLOT["left%d" % hp]], right) for hp in range(PAIRS)])
        rc_ql.append([remote(own[hp], qall.at[SLOT["right%d" % hp]], left) for hp in range(PAIRS)])
        fwd = []
        for hp in range(PAIRS):
            side, dev = ("left", right) if hp % 2 == 0 else ("right", left)
            fwd.append(remote(qall.at[SLOT["%s%d" % (side, hp)]], qall.at[SLOT["opp%d" % hp]], dev))
        rc_qf.append(fwd)
        outs = {}
        for hp in range(PAIRS):
            outs["left%d" % hp] = remote(obuf.at[SLOT["left%d" % hp]], final.at[1, hp], left)
            outs["right%d" % hp] = remote(obuf.at[SLOT["right%d" % hp]], final.at[0, hp], right)
            outs["opp%d" % hp] = remote(obuf.at[SLOT["opp%d" % hp]], relay.at[hp], right if hp % 2 == 0 else left)
        rc_o.append(outs)
    rc_y1 = [remote(ysend.at[n], yrecv.at[n], partner) for n in range(ncol)]
    other_rows = pl.ds(pl.multiple_of((1 - core) * tok, tok), tok)
    rc_y2 = [remote(ysend.at[n, other_rows], yrecv.at[n, pl.ds(0, tok)], partner) for n in range(ncol)]
    rc_m = [remote(macc.at[n], mrecv.at[n], partner) for n in range(ncol)]

    ff_half = w_gate.shape[1] // 2
    nfull = (ff_half - ff_first) // ff_chunk
    tail = ff_half - ff_first - nfull * ff_chunk

    def ff_copies(chunk, slot, size):
        cols = pl.ds(pl.multiple_of(core * ff_half + ff_first + chunk * ff_chunk, 128), size)
        return (pltpu.make_async_copy(w_gate.at[:, cols], w1s.at[slot, :, pl.ds(0, size)], rings.at[0, slot]),
                pltpu.make_async_copy(w_up.at[:, cols], w3s.at[slot, :, pl.ds(0, size)], rings.at[1, slot]),
                pltpu.make_async_copy(w_down.at[cols], w2s.at[slot, pl.ds(0, size)], rings.at[2, slot]))

    def rope(val, la_bias, cos_v, sin_v):
        val = (val + la_bias).astype(BF16).astype(F32)
        return (val * cos_v + pltpu.roll(val, hd // 2, 1) * sin_v).astype(BF16)

    def prep_cache(la):
        if la == 1:
            rc_k[0].wait_send()
            rc_v[0].wait_send()
        blk = deint.shape[0] // 2

        def split(ref, i):
            deint[...] = ref[pl.ds(pl.multiple_of(i * 2 * blk, 2 * blk), 2 * blk), :].astype(F32)
            head0 = deint[pl.ds(0, blk, stride=2), :]
            head1 = deint[pl.ds(1, blk, stride=2), :]
            is0 = core == 0
            return jnp.where(is0, head0, head1), jnp.where(is0, head1, head0)

        def kbody(i, _):
            mine, other = split(kstage, i)
            at = pl.ds(pl.multiple_of(i * blk, blk), blk)
            kall[la, at, :] = mine.astype(BF16)
            ksend[at, :] = other.astype(BF16)
            return 0

        def vbody(i, _):
            mine, other = split(vstage, i)
            at = pl.ds(pl.multiple_of(i * blk, blk), blk)
            vtall[la, :, at] = mine.T.astype(BF16)
            vsend[:, at] = other.T.astype(BF16)
            return 0

        cp_ks[la].wait()
        lax.fori_loop(0, keys_dev // blk, kbody, 0)
        rc_k[la].start()
        cp_vs[la].wait()
        lax.fori_loop(0, keys_dev // blk, vbody, 0)
        rc_v[la].start()
        if la == 0:
            cp_ks[1].start()
            cp_vs[1].start()

    def project(la, in_ref):
        heads_half = half_w // hd
        bq_v = bqb[la].astype(F32)
        bq_v = jnp.where(core == 0, bq_v[:heads_half], bq_v[heads_half:])
        bk_v = bkb[la].astype(F32)
        cos_v, sin_v = cosb[...], sinb[...]
        for half in range(2):
            cp_wq[la][half].wait()
            acc = jnp.dot(in_ref[...], wqb[half][...], preferred_element_type=F32)
            for hp in (2 * half, 2 * half + 1):
                slot = SLOT["own%d" % hp]
                for j in range(2):
                    row = hp * 2 + j
                    at = (row - 4 * half) * hd
                    qall[slot, pl.ds(j * ctok, ctok), :] = rope(acc[:, at:at + hd], bq_v[row:row + 1], cos_v, sin_v)
                rc_qr[la][hp].start()
                rc_ql[la][hp].start()
        cp_wk[la].wait()
        cp_wv[la].wait()
        acc = jnp.dot(in_ref[...], wkvb[...], preferred_element_type=F32)
        k_heads = [rope(acc[:, j * hd:(j + 1) * hd], bk_v[j:j + 1], cos_v, sin_v).astype(F32) for j in range(2)]
        acc = acc[:, 2 * hd:]
        v_heads = [acc[:, j * hd:(j + 1) * hd].astype(BF16).astype(F32) for j in range(2)]
        is0 = core == 0
        kall[la, pl.ds(keys_chip, ctok), :] = jnp.where(is0, k_heads[0], k_heads[1]).astype(BF16)
        vtall[la, :, pl.ds(keys_chip, ctok)] = jnp.where(is0, v_heads[0], v_heads[1]).T.astype(BF16)
        for which, heads in ((0, k_heads), (1, v_heads)):
            for j in range(2):
                mine = jnp.where(is0, heads[j][:tok], heads[j][tok:])
                deint[pl.ds(j, tok, stride=2), :] = mine
            kvout[la, which] = deint[pl.ds(0, 2 * tok), :].astype(BF16)
        cp_kout[la].start()
        cp_vout[la].start()

    offs = {"own": 0, "left": (left_chip - chip) * ctok, "right": (right_chip - chip) * ctok, "opp": (opp_chip - chip) * ctok}

    def unit_offset(unit):
        res = jnp.int32(0)
        for name, idx in SLOT.items():
            if not name.startswith("own"):
                res = jnp.where(unit == idx, offs[name[:-1]], res)
        return res

    def scores(la, unit, s_ref, m_ref):
        s_val = lax.dot_general(kall[la], qall[unit], (((1,), (1,)), ((), ())), preferred_element_type=F32)
        s_ref[pl.ds(0, keys_chip), :] = s_val[:keys_chip]
        peak = jnp.max(s_val[:keys_chip].reshape(keys_chip // 8, 8, rows), axis=0)
        key_i = lax.broadcasted_iota(jnp.int32, (ctok, rows), 0)
        tok_i = lax.broadcasted_iota(jnp.int32, (ctok, rows), 1) % ctok
        masked = jnp.where(key_i - tok_i <= unit_offset(unit), s_val[keys_chip:], -jnp.inf)
        s_ref[pl.ds(keys_chip, ctok), :] = masked
        m_ref[...] = jnp.maximum(peak, jnp.max(masked.reshape(ctok // 8, 8, rows), axis=0))

    row8 = lax.broadcasted_iota(jnp.int32, (8, ctok), 0)

    def put(dst, heads):
        for h, (out_v, _, _) in enumerate(heads):
            dst[pl.ds(h * hd, hd), :] = out_v
        (_, peak0, total0), (_, peak1, total1) = heads
        dst[pl.ds(2 * hd, 8), :] = jnp.where(row8 == 0, peak0, jnp.where(row8 == 1, peak1, jnp.where(row8 == 2, total0, total1)))

    def get(src):
        return [(src[pl.ds(h * hd, hd), :], src[pl.ds(2 * hd + h, 1), :], src[pl.ds(2 * hd + 2 + h, 1), :]) for h in range(2)]

    def merged(parts):
        peak = functools.reduce(jnp.maximum, [part[1] for part in parts])
        scales = [jnp.exp2((part[1] - peak) * cexp) for part in parts]
        out_v = functools.reduce(jnp.add, [part[0] * sc for part, sc in zip(parts, scales)])
        total = functools.reduce(jnp.add, [part[2] * sc for part, sc in zip(parts, scales)])
        return out_v, peak, total

    def merged_heads(refs):
        return [merged(parts) for parts in zip(*[get(ref) for ref in refs])]

    def attend_unit(la, unit, nxt, s_cur, m_cur, s_nxt, m_nxt):
        peak = jnp.max(m_cur[...], axis=0, keepdims=True)
        shift = jnp.broadcast_to(peak * cexp, (8, rows))
        prob = jnp.exp2(s_cur[...].reshape(keys_tot // 8, 8, rows) * cexp - shift[None])
        total = jnp.sum(jnp.sum(prob, axis=0), axis=0, keepdims=True)
        out_v = jnp.dot(vtall[la], prob.reshape(keys_tot, rows).astype(BF16), preferred_element_type=F32)
        scores(la, nxt, s_nxt, m_nxt)
        put(obuf.at[unit], [tuple(val[:, h * ctok:(h + 1) * ctok] for val in (out_v, peak, total)) for h in range(2)])

    def before(la):
        acts = {}

        def add(name, *fns):
            acts.setdefault(SLOT[name] - 1, []).extend(fns)

        for hp in range(PAIRS):
            lw, rw = rc_qr[la][hp].wait_recv, rc_ql[la][hp].wait_recv
            fwd = rc_qf[la][hp]
            if hp % 2 == 0:
                acts.setdefault(FORWARD_BEFORE[hp], []).extend([lw, fwd.start])
                add("right%d" % hp, rw)
            else:
                acts.setdefault(FORWARD_BEFORE[hp], []).extend([rw, fwd.start])
                add("left%d" % hp, lw)
        for hp in range(PAIRS):
            add("opp%d" % hp, rc_qf[la][hp].wait_recv)
        return acts

    def after(la):
        acts = {}
        for name, cp in rc_o[la].items():
            hp = int(name[-1])
            merge_it = (name.startswith("right") and hp % 2 == 0) or (name.startswith("left") and hp % 2 == 1)

            def act(name=name, cp=cp, hp=hp, merge_it=merge_it):
                if name.startswith("left" if hp % 2 == 0 else "right"):
                    rc_qf[la][hp].wait_send()
                if merge_it:
                    rc_o[la]["opp%d" % hp].wait_recv()
                    put(obuf.at[SLOT[name]], merged_heads([obuf.at[SLOT[name]], relay.at[hp]]))
                cp.start()

            acts[SLOT[name]] = [act]
        return acts

    def attention(la):
        pl.run_scoped(functools.partial(attend_all, la), pltpu.VMEM((keys_tot, rows), F32), pltpu.VMEM((keys_tot, rows), F32))

    def attend_all(la, s_a, s_b):
        rc_k[la].wait_recv()
        rc_v[la].wait_recv()
        with scope("score0"):
            scores(la, 0, s_a, m_a)
        pre, post = before(la), after(la)

        def run(acts, pair, parity):
            for unit, fns in acts.items():
                if unit % 2 == parity:
                    @pl.when(pair == unit // 2)
                    def _(fns=fns):
                        with scope("event"):
                            for fn in fns:
                                fn()

        def body(pair, _):
            run(pre, pair, 0)
            attend_unit(la, 2 * pair, 2 * pair + 1, s_a, m_a, s_b, m_b)
            run(post, pair, 0)
            run(pre, pair, 1)
            attend_unit(la, 2 * pair + 1, jnp.minimum(2 * pair + 2, UNITS - 1), s_b, m_b, s_a, m_a)
            run(post, pair, 1)
            return 0

        lax.fori_loop(0, UNITS // 2, body, 0)

    def finish_attention(la):
        for hp in range(PAIRS):
            with scope("owait"):
                rc_o[la]["right%d" % hp].wait_recv()
                rc_o[la]["left%d" % hp].wait_recv()
            heads = merged_heads([obuf.at[SLOT["own%d" % hp]], final.at[0, hp], final.at[1, hp]])
            for h, (out_v, _, total) in enumerate(heads):
                ohalf[:, pl.ds((2 * hp + h) * hd, hd)] = (out_v / total).T.astype(BF16)
        cp_wo[la].wait()
        rc_y = (rc_y1, rc_y2)[la]
        for n in range(ncol):
            ysend[n] = jnp.dot(ohalf[...], wob[:, n * cw:(n + 1) * cw], preferred_element_type=F32)
            rc_y[n].start()
        for cp in list(rc_qr[la]) + list(rc_ql[la]) + list(rc_o[la].values()):
            cp.wait_send()

    def normed(wide):
        return (wide * lax.rsqrt(jnp.mean(wide * wide, axis=-1, keepdims=True) + NORM_EPS)).astype(BF16)

    def row_loop(count, fn):
        def body(i, _):
            fn(pl.ds(pl.multiple_of(i * NORM_ROWS, NORM_ROWS), NORM_ROWS))
            return 0

        lax.fori_loop(0, count // NORM_ROWS, body, 0)

    cp_x.start()
    cp_cos.start()
    cp_sin.start()
    for cp in cp_bq + cp_bk:
        cp.start()
    cp_ks[0].start()
    cp_vs[0].start()
    for half in range(2):
        cp_wq[0][half].start()
    cp_wk[0].start()
    cp_wv[0].start()
    with scope("entry"):
        pl.semaphore_wait(barrier, 3)
    rc_x.start()
    with scope("prep0"):
        prep_cache(0)
    cp_cos.wait()
    cp_sin.wait()
    for cp in cp_bq + cp_bk:
        cp.wait()
    cp_x.wait()
    with scope("xwait"):
        rc_x.wait_recv()
    with scope("proj0"):
        project(0, xbuf)
    cp_wo[0].start()
    cp_wk[1].start()
    cp_wv[1].start()
    for slot in range(ff_slots):
        for cp in ff_copies(slot, slot, ff_chunk):
            cp.start()
    with scope("attn0"):
        attention(0)
    def middle(w1f, w3f, w2f):
        cols = pl.ds(pl.multiple_of(core * ff_half, 128), ff_first)
        cp_first = [local(w_gate.at[:, cols], w1f), local(w_up.at[:, cols], w3f), local(w_down.at[cols], w2f)]
        for cp in cp_first:
            cp.start()
        with scope("prep1"):
            prep_cache(1)
        with scope("fin0"):
            finish_attention(0)
        with scope("ywait"):
            for n in range(ncol):
                rc_y1[n].wait()

        def first_norm(rs):
            parts = [(ysend[n, rs, :] + yrecv[n, rs, :]).astype(BF16).astype(F32) for n in range(ncol)]
            res = (xbuf[rs, :].astype(F32) + jnp.concatenate(parts, axis=1)).astype(BF16)
            hbuf[rs, :] = res
            ubuf[rs, :] = normed(res.astype(F32))

        with scope("norm1"):
            row_loop(ctok, first_norm)

        def gate_up(w1, w3):
            gate = jnp.dot(ubuf[...], w1[...], preferred_element_type=F32).astype(BF16).astype(F32)
            up = jnp.dot(ubuf[...], w3[...], preferred_element_type=F32).astype(BF16).astype(F32)
            return (jax.nn.silu(gate) * up).astype(BF16)

        def down(w2, size, init=False, send=False):
            for n in range(ncol):
                part = jnp.dot(ebuf[:, pl.ds(0, size)], w2[:, pl.ds(n * cw, cw)], preferred_element_type=F32)
                if init:
                    macc[n] = part
                else:
                    macc[n] += part
                if send:
                    rc_m[n].start()

        def ring_up(slot, size):
            return gate_up(w1s.at[slot, :, pl.ds(0, size)], w3s.at[slot, :, pl.ds(0, size)])

        def ring_down(slot, size, send=False):
            down(w2s.at[slot, pl.ds(0, size)], size, send=send)

        def refill(chunk, which):
            for size, cond in ((ff_chunk, chunk < nfull), (tail, chunk == nfull)):
                if size:
                    @pl.when(cond)
                    def _(size=size):
                        cps = ff_copies(chunk, lax.rem(chunk, ff_slots), size)
                        for w in which:
                            cps[w].start()

        with scope("mlp_a"):
            cp_first[0].wait()
            cp_first[1].wait()
            ebuf[:, pl.ds(0, ff_first)] = gate_up(w1f, w3f)
            ready = ff_copies(0, 0, ff_chunk)
            ready[0].wait()
            ready[1].wait()
            cp_first[2].wait()
            hidden = ring_up(0, ff_chunk)
            down(w2f, ff_first, init=True)
            ebuf[:, pl.ds(0, ff_chunk)] = hidden
            refill(jnp.int32(ff_slots), (0, 1))

        def mlp_body(k, _):
            slot, prev = lax.rem(k, ff_slots), lax.rem(k - 1, ff_slots)
            cps = ff_copies(k, slot, ff_chunk)
            with scope("stream"):
                cps[0].wait()
                cps[1].wait()
                ff_copies(k - 1, prev, ff_chunk)[2].wait()
            hidden = ring_up(slot, ff_chunk)
            ring_down(prev, ff_chunk)
            ebuf[:, pl.ds(0, ff_chunk)] = hidden
            refill(k + ff_slots, (0, 1))
            refill(k - 1 + ff_slots, (2,))
            return 0

        with scope("mlp"):
            lax.fori_loop(1, nfull, mlp_body, 0)
        last_slot = (nfull - 1) % ff_slots
        with scope("mlp_z"):
            ff_copies(nfull - 1, last_slot, ff_chunk)[2].wait()
            if tail:
                slot = nfull % ff_slots
                cps = ff_copies(nfull, slot, tail)
                cps[0].wait()
                cps[1].wait()
                hidden = ring_up(slot, tail)
                ring_down(last_slot, ff_chunk)
                ebuf[:, pl.ds(0, tail)] = hidden
                for half in range(2):
                    cp_wq[1][half].start()
                cps[2].wait()
                ring_down(slot, tail, send=True)
            else:
                for half in range(2):
                    cp_wq[1][half].start()
                ring_down(last_slot, ff_chunk, send=True)
            cp_wo[1].start()
        with scope("mwait"):
            for n in range(ncol):
                rc_m[n].wait()

        def second_norm(rs):
            acc = jnp.concatenate([macc[n, rs, :] + mrecv[n, rs, :] for n in range(ncol)], axis=1)
            res = (hbuf[rs, :].astype(F32) + acc).astype(BF16)
            hbuf[rs, :] = res
            ubuf[rs, :] = normed(res.astype(F32))

        with scope("norm2"):
            row_loop(ctok, second_norm)
        gout[0] = hbuf[my_rows, :]
        cp_g.start()

    pl.run_scoped(middle, pltpu.VMEM((width, ff_first), BF16), pltpu.VMEM((width, ff_first), BF16),
                  pltpu.VMEM((ff_first, width), BF16))
    with scope("proj1"):
        project(1, ubuf)
    with scope("attn1"):
        attention(1)
    with scope("fin1"):
        finish_attention(1)
    for n in range(ncol):
        rc_y2[n].wait()
        gout[1, :, pl.ds(n * cw, cw)] = (ysend[n, my_rows, :] + yrecv[n, pl.ds(0, tok), :]).astype(BF16)
    cp_y.start()
    rc_x.wait_send()
    rc_k[1].wait_send()
    rc_v[1].wait_send()
    for cp in cp_kout + cp_vout + [cp_g, cp_y]:
        cp.wait()


def copy_out(*refs):
    half = len(refs) // 2
    for src, dst in zip(refs[:half], refs[half:]):
        dst[...] = src[...]


def solution(mesh):
    axis_size = mesh.shape["cp"]
    nchip = axis_size // 2
    ff_first, ff_chunk, ff_slots = 384, 512, 5
    rows_spec = P(("dp", "cp"), None)
    cache_spec = P(("dp", "cp"), None, None)
    mat_spec = P(None, None)
    vec_spec = P(None)
    layer_specs = (cache_spec, cache_spec, mat_spec, vec_spec, mat_spec, vec_spec, mat_spec, mat_spec)
    in_specs = (rows_spec,) + layer_specs + (mat_spec, mat_spec, mat_spec) + layer_specs
    out_specs = (rows_spec, rows_spec, cache_spec, cache_spec, cache_spec, cache_spec)

    def forward(x_in, cache_k1, cache_v1, w_q1, b_q1, w_k1, b_k1, w_v1, w_o1, w_gate, w_up, w_down,
                cache_k2, cache_v2, w_q2, b_q2, w_k2, b_k2, w_v2, w_o2):
        tok, width = x_in.shape
        cache_dev, kv_heads, hd = cache_k1.shape
        ctok = 2 * tok
        rows = 2 * ctok
        keys_tot = 2 * cache_dev + ctok
        cos_t, sin_t = rope_tables(axis_size * cache_dev, axis_size * tok, hd)
        flat = lambda arr: arr.reshape(-1, hd)
        half_w = width // 2
        ncol = 4
        hbm = pl.BlockSpec(memory_space=pl.ANY)
        scratch = [
            pltpu.VMEM((ctok, width), BF16),
            pltpu.VMEM((ctok, width), BF16),
            pltpu.VMEM((ctok, width), BF16),
            pltpu.VMEM((width, 4 * hd), BF16),
            pltpu.VMEM((half_w, width), BF16),
            pltpu.VMEM((2, keys_tot, hd), BF16),
            pltpu.VMEM((2, hd, keys_tot), BF16),
            pltpu.VMEM((2 * cache_dev, hd), BF16),
            pltpu.VMEM((2 * cache_dev, hd), BF16),
            pltpu.VMEM((cache_dev, hd), BF16),
            pltpu.VMEM((hd, cache_dev), BF16),
            pltpu.VMEM((8 * hd, hd), F32),
            pltpu.VMEM((UNITS, rows, hd), BF16),
            pltpu.VMEM((8, rows), F32),
            pltpu.VMEM((8, rows), F32),
            pltpu.VMEM((UNITS, 2 * hd + 8, ctok), F32),
            pltpu.VMEM((PAIRS, 2 * hd + 8, ctok), F32),
            pltpu.VMEM((2, PAIRS, 2 * hd + 8, ctok), F32),
            pltpu.VMEM((ctok, half_w), BF16),
            pltpu.VMEM((ncol, ctok, width // ncol), F32),
            pltpu.VMEM((ncol, ctok, width // ncol), F32),
            pltpu.VMEM((ncol, ctok, width // ncol), F32),
            pltpu.VMEM((ff_slots, width, ff_chunk), BF16),
            pltpu.VMEM((ff_slots, width, ff_chunk), BF16),
            pltpu.VMEM((ff_slots, ff_chunk, width), BF16),
            pltpu.VMEM((ctok, max(ff_first, ff_chunk)), BF16),
            pltpu.VMEM((ctok, hd), F32),
            pltpu.VMEM((ctok, hd), F32),
            pltpu.VMEM((2, width // hd, hd), BF16),
            pltpu.VMEM((2, kv_heads, hd), BF16),
            pltpu.VMEM((2, 2, 2 * tok, hd), BF16),
            pltpu.VMEM((2, tok, width), BF16),
            pltpu.SemaphoreType.DMA((32,)),
            pltpu.SemaphoreType.DMA((3, ff_slots)),
            pltpu.SemaphoreType.DMA((65,)),
            pltpu.SemaphoreType.DMA((65,)),
        ]
        act = jax.ShapeDtypeStruct((tok, width), BF16)
        app = jax.ShapeDtypeStruct((kv_heads * tok, hd), BF16)
        outs = pl.pallas_call(
            functools.partial(block_kernel, nchip, ff_first, ff_chunk, ff_slots),
            out_shape=(act, act, app, app, app, app),
            in_specs=[hbm] * 22,
            out_specs=(hbm,) * 6,
            scratch_shapes=scratch,
            compiler_params=pltpu.CompilerParams(collective_id=0, has_side_effects=True, vmem_limit_bytes=67043328),
        )(x_in, flat(cache_k1), flat(cache_v1), w_q1, w_k1, w_v1, w_o1, w_gate, w_up, w_down,
          flat(cache_k2), flat(cache_v2), w_q2, w_k2, w_v2, w_o2,
          flat(b_q1), flat(b_k1), flat(b_q2), flat(b_k2), jnp.asarray(cos_t), jnp.asarray(sin_t))
        outs = pl.pallas_call(copy_out, out_shape=[jax.ShapeDtypeStruct(arr.shape, arr.dtype) for arr in outs])(*outs)
        hidden, y_two = outs[:2]
        appends = [arr.reshape(tok, kv_heads, hd) for arr in outs[2:]]
        return (hidden, y_two, *appends)

    return jax.shard_map(forward, mesh=mesh, in_specs=in_specs, out_specs=out_specs, check_vma=False)
```

```python
import functools
import math

import jax
import jax.numpy as jnp
import numpy as np
from jax import lax
from jax.experimental import pallas as pl
from jax.experimental.pallas import tpu as pltpu
from jax.sharding import PartitionSpec as P

ROPE_THETA = 500000.0
NORM_EPS = 1e-5
MESH = pl.DeviceIdType.MESH
scope = jax.named_scope
F32 = jnp.float32
BF16 = jnp.bfloat16

ORDER = ("own0", "own1", "left0", "right1", "left2", "opp0", "opp1", "right3", "opp2", "opp3",
         "right0", "left1", "own2", "right2", "left3", "own3")
FORWARD_BEFORE = (1, 2, 3, 4)
SLOT = {name: idx for idx, name in enumerate(ORDER)}
UNITS = len(ORDER)
PAIRS = 4
NORM_ROWS = 32


def rope_tables(first_pos, count, head_dim):
    half_dim = head_dim // 2
    exponent = np.arange(half_dim, dtype=np.float32) * np.float32(2.0 / head_dim)
    inv_freq = (np.float32(1.0) / np.power(np.float32(ROPE_THETA), exponent)).astype(np.float32)
    positions = (first_pos + np.arange(count)).astype(np.float32)
    angles = (positions[:, None] * inv_freq[None, :]).astype(np.float32)
    cos_t = np.cos(angles.astype(np.float64)).astype(np.float32)
    sin_t = np.sin(angles.astype(np.float64)).astype(np.float32)
    return np.concatenate([cos_t, cos_t], axis=1), np.concatenate([-sin_t, sin_t], axis=1)


def block_kernel(nchip, ff_first, ff_chunk, ff_slots,
                 x_hbm, kc1, vc1, wq1, wk1, wv1, wo1, w_gate, w_up, w_down, kc2, vc2, wq2, wk2, wv2, wo2,
                 bq1, bk1, bq2, bk2, cos_hbm, sin_hbm,
                 g_out, y_out, k1_out, v1_out, k2_out, v2_out,
                 xbuf, hbuf, ubuf, wkvb, wob, kall, vtall, ksend, vsend, deint,
                 qall, m_a, m_b, obuf, relay, final, ohalf, ysend, yrecv, mrecv,
                 w1s, w3s, w2s, ebuf, cosb, sinb, bqb, bkb, kvout, gout,
                 dsem, rings, ssem, rsem):
    tok = x_hbm.shape[0]
    ctok = 2 * tok
    width = x_hbm.shape[1]
    hd = kc1.shape[1]
    keys_dev = kc1.shape[0] // 2
    keys_chip = 2 * keys_dev
    keys_tot = keys_chip + ctok
    rows = 2 * ctok
    half_w = width // 2
    ncol = 4
    cw = width // ncol
    cexp = math.log2(math.e) / math.sqrt(hd)

    me = lax.axis_index("cp")
    chip = me // 2
    core = lax.rem(me, 2)
    partner = chip * 2 + 1 - core
    left_chip = lax.rem(chip + nchip - 1, nchip)
    right_chip = lax.rem(chip + 1, nchip)
    opp_chip = lax.rem(chip + 2, nchip)
    left = left_chip * 2 + core
    right = right_chip * 2 + core

    macc = ysend
    dcount = [0]

    def local(src, dst):
        idx = dcount[0]
        dcount[0] += 1
        return pltpu.make_async_copy(src, dst, dsem.at[idx])

    rcount = [0]

    def remote(src, dst, dev):
        idx = rcount[0]
        rcount[0] += 1
        return pltpu.make_async_remote_copy(src_ref=src, dst_ref=dst, send_sem=ssem.at[idx], recv_sem=rsem.at[idx],
                                            device_id={"cp": dev}, device_id_type=MESH)

    barrier = pltpu.get_barrier_semaphore()
    for dev in (partner, left, right):
        pl.semaphore_signal(barrier, inc=1, device_id={"cp": dev}, device_id_type=MESH)

    my_rows = pl.ds(pl.multiple_of(core * tok, tok), tok)
    kc = (kc1, kc2)
    vc = (vc1, vc2)
    wq = (wq1, wq2)
    wk = (wk1, wk2)
    wv = (wv1, wv2)
    wo = (wo1, wo2)
    k_out = (k1_out, k2_out)
    v_out = (v1_out, v2_out)

    cp_x = local(x_hbm, xbuf.at[my_rows])
    pos_rows = pl.ds(pl.multiple_of(chip * ctok, ctok), ctok)
    cp_cos = local(cos_hbm.at[pos_rows], cosb)
    cp_sin = local(sin_hbm.at[pos_rows], sinb)
    cp_bq = [local(ref, bqb.at[la]) for la, ref in enumerate((bq1, bq2))]
    cp_bk = [local(ref, bkb.at[la]) for la, ref in enumerate((bk1, bk2))]
    qcol = [pl.ds(pl.multiple_of(core * half_w + half * 2 * rows, rows), 2 * rows) for half in range(2)]
    wqb = [ref.at[ff_slots - 1, :, pl.ds(0, 2 * rows)] for ref in (w1s, w3s)]
    cp_wq = [[local(wq[la].at[:, qcol[half]], wqb[half]) for half in range(2)] for la in range(2)]
    cp_wk = [local(wk[la], wkvb.at[:, pl.ds(0, 2 * hd)]) for la in range(2)]
    cp_wv = [local(wv[la], wkvb.at[:, pl.ds(2 * hd, 2 * hd)]) for la in range(2)]
    cp_wo = [local(wo[la].at[pl.ds(pl.multiple_of(core * half_w, half_w), half_w)], wob) for la in range(2)]
    cp_kout = [local(kvout.at[la, 0], k_out[la]) for la in range(2)]
    cp_vout = [local(kvout.at[la, 1], v_out[la]) for la in range(2)]
    cp_g = local(gout.at[0], g_out)
    cp_y = [local(gout.at[1, :, pl.ds(n * cw, cw)], y_out.at[:, pl.ds(n * cw, cw)]) for n in range(ncol)]

    rc_x = remote(x_hbm, xbuf.at[my_rows], partner)
    rc_k = [remote(ksend, kall.at[la, pl.ds(keys_dev, keys_dev)], partner) for la in range(2)]
    rc_v = [remote(vsend, vtall.at[la, :, pl.ds(keys_dev, keys_dev)], partner) for la in range(2)]
    rc_qr, rc_ql, rc_qf, rc_o = [], [], [], []
    for la in range(2):
        own = [qall.at[SLOT["own%d" % hp]] for hp in range(PAIRS)]
        rc_qr.append([remote(own[hp], qall.at[SLOT["left%d" % hp]], right) for hp in range(PAIRS)])
        rc_ql.append([remote(own[hp], qall.at[SLOT["right%d" % hp]], left) for hp in range(PAIRS)])
        fwd = []
        for hp in range(PAIRS):
            side, dev = ("left", right) if hp % 2 == 0 else ("right", left)
            fwd.append(remote(qall.at[SLOT["%s%d" % (side, hp)]], qall.at[SLOT["opp%d" % hp]], dev))
        rc_qf.append(fwd)
        outs = {}
        for hp in range(PAIRS):
            outs["left%d" % hp] = remote(obuf.at[SLOT["left%d" % hp]], final.at[1, hp], left)
            outs["right%d" % hp] = remote(obuf.at[SLOT["right%d" % hp]], final.at[0, hp], right)
            outs["opp%d" % hp] = remote(obuf.at[SLOT["opp%d" % hp]], relay.at[hp], right if hp % 2 == 0 else left)
        rc_o.append(outs)
    rc_y1 = [remote(ysend.at[n], yrecv.at[n], partner) for n in range(ncol)]
    other_rows = pl.ds(pl.multiple_of((1 - core) * tok, tok), tok)
    rc_y2 = [remote(ysend.at[n, other_rows], yrecv.at[n, pl.ds(0, tok)], partner) for n in range(ncol)]
    rc_m = [remote(macc.at[n], mrecv.at[n], partner) for n in range(ncol)]

    ff_half = w_gate.shape[1] // 2
    nfull = (ff_half - ff_first) // ff_chunk
    assert ff_half == ff_first + nfull * ff_chunk and nfull > ff_slots

    def ff_copies(chunk, slot, size):
        cols = pl.ds(pl.multiple_of(core * ff_half + ff_first + chunk * ff_chunk, 128), size)
        return (pltpu.make_async_copy(w_gate.at[:, cols], w1s.at[slot, :, pl.ds(0, size)], rings.at[0, slot]),
                pltpu.make_async_copy(w_up.at[:, cols], w3s.at[slot, :, pl.ds(0, size)], rings.at[1, slot]),
                pltpu.make_async_copy(w_down.at[cols], w2s.at[slot, pl.ds(0, size)], rings.at[2, slot]))

    def rope(val, la_bias, cos_v, sin_v):
        val = (val + la_bias).astype(BF16).astype(F32)
        return (val * cos_v + pltpu.roll(val, hd // 2, 1) * sin_v).astype(BF16)

    stages = [pltpu.VMEM(kc1.shape, BF16), pltpu.VMEM(vc1.shape, BF16)]

    def stage_cache(la, kstage, vstage):
        cps = local(kc[la], kstage), local(vc[la], vstage)
        for cp in cps:
            cp.start()
        return cps

    def prep_cache(la, kstage, vstage, cps):
        if la == 1:
            rc_k[0].wait_send()
            rc_v[0].wait_send()
        blk = deint.shape[0] // 2

        def split(ref, i):
            deint[...] = ref[pl.ds(pl.multiple_of(i * 2 * blk, 2 * blk), 2 * blk), :].astype(F32)
            head0 = deint[pl.ds(0, blk, stride=2), :]
            head1 = deint[pl.ds(1, blk, stride=2), :]
            is0 = core == 0
            return jnp.where(is0, head0, head1), jnp.where(is0, head1, head0)

        def kbody(i, _):
            mine, other = split(kstage, i)
            at = pl.ds(pl.multiple_of(i * blk, blk), blk)
            kall[la, at, :] = mine.astype(BF16)
            ksend[at, :] = other.astype(BF16)
            return 0

        def vbody(i, _):
            mine, other = split(vstage, i)
            at = pl.ds(pl.multiple_of(i * blk, blk), blk)
            vtall[la, :, at] = mine.T.astype(BF16)
            vsend[:, at] = other.T.astype(BF16)
            return 0

        cps[0].wait()
        lax.fori_loop(0, keys_dev // blk, kbody, 0)
        rc_k[la].start()
        cps[1].wait()
        lax.fori_loop(0, keys_dev // blk, vbody, 0)
        rc_v[la].start()

    def project(la, in_ref):
        heads_half = half_w // hd
        bq_v = bqb[la].astype(F32)
        bq_v = jnp.where(core == 0, bq_v[:heads_half], bq_v[heads_half:])
        bk_v = bkb[la].astype(F32)
        cos_v, sin_v = cosb[...], sinb[...]
        for half in range(2):
            cp_wq[la][half].wait()
            acc = jnp.dot(in_ref[...], wqb[half][...], preferred_element_type=F32)
            for hp in (2 * half, 2 * half + 1):
                slot = SLOT["own%d" % hp]
                for j in range(2):
                    row = hp * 2 + j
                    at = (row - 4 * half) * hd
                    qall[slot, pl.ds(j * ctok, ctok), :] = rope(acc[:, at:at + hd], bq_v[row:row + 1], cos_v, sin_v)
                rc_qr[la][hp].start()
                rc_ql[la][hp].start()
        cp_wk[la].wait()
        cp_wv[la].wait()
        acc = jnp.dot(in_ref[...], wkvb[...], preferred_element_type=F32)
        k_heads = [rope(acc[:, j * hd:(j + 1) * hd], bk_v[j:j + 1], cos_v, sin_v).astype(F32) for j in range(2)]
        acc = acc[:, 2 * hd:]
        v_heads = [acc[:, j * hd:(j + 1) * hd].astype(BF16).astype(F32) for j in range(2)]
        is0 = core == 0
        kall[la, pl.ds(keys_chip, ctok), :] = jnp.where(is0, k_heads[0], k_heads[1]).astype(BF16)
        vtall[la, :, pl.ds(keys_chip, ctok)] = jnp.where(is0, v_heads[0], v_heads[1]).T.astype(BF16)
        for which, heads in ((0, k_heads), (1, v_heads)):
            for j in range(2):
                mine = jnp.where(is0, heads[j][:tok], heads[j][tok:])
                deint[pl.ds(j, tok, stride=2), :] = mine
            kvout[la, which] = deint[pl.ds(0, 2 * tok), :].astype(BF16)
        cp_kout[la].start()
        cp_vout[la].start()

    offs = {"own": 0, "left": (left_chip - chip) * ctok, "right": (right_chip - chip) * ctok, "opp": (opp_chip - chip) * ctok}

    def unit_offset(unit):
        res = jnp.int32(0)
        for name, idx in SLOT.items():
            if not name.startswith("own"):
                res = jnp.where(unit == idx, offs[name[:-1]], res)
        return res

    def scores(la, unit, s_ref, m_ref):
        s_val = lax.dot_general(kall[la], qall[unit], (((1,), (1,)), ((), ())), preferred_element_type=F32) * cexp
        s_ref[pl.ds(0, keys_chip), :] = s_val[:keys_chip]
        peak = jnp.max(s_val[:keys_chip].reshape(keys_chip // 8, 8, rows), axis=0)
        key_i = lax.broadcasted_iota(jnp.int32, (ctok, rows), 0)
        tok_i = lax.broadcasted_iota(jnp.int32, (ctok, rows), 1) % ctok
        masked = jnp.where(key_i - tok_i <= unit_offset(unit), s_val[keys_chip:], -jnp.inf)
        s_ref[pl.ds(keys_chip, ctok), :] = masked
        m_ref[...] = jnp.maximum(peak, jnp.max(masked.reshape(ctok // 8, 8, rows), axis=0))

    row8 = lax.broadcasted_iota(jnp.int32, (8, ctok), 0)

    def put(dst, heads):
        for h, (out_v, _, _) in enumerate(heads):
            dst[pl.ds(h * hd, hd), :] = out_v
        (_, peak0, total0), (_, peak1, total1) = heads
        dst[pl.ds(2 * hd, 8), :] = jnp.where(row8 == 0, peak0, jnp.where(row8 == 1, peak1, jnp.where(row8 == 2, total0, total1)))

    def get(src):
        return [(src[pl.ds(h * hd, hd), :], src[pl.ds(2 * hd + h, 1), :], src[pl.ds(2 * hd + 2 + h, 1), :]) for h in range(2)]

    def merged(parts):
        peak = functools.reduce(jnp.maximum, [part[1] for part in parts])
        scales = [jnp.exp2(part[1] - peak) for part in parts]
        out_v = functools.reduce(jnp.add, [part[0] * sc for part, sc in zip(parts, scales)])
        total = functools.reduce(jnp.add, [part[2] * sc for part, sc in zip(parts, scales)])
        return out_v, peak, total

    def merged_heads(refs):
        return [merged(parts) for parts in zip(*[get(ref) for ref in refs])]

    def attend_unit(la, unit, nxt, s_cur, m_cur, s_nxt, m_nxt):
        peak = jnp.max(m_cur[...], axis=0, keepdims=True)
        shift = jnp.broadcast_to(peak, (8, rows))
        prob = jnp.exp2(s_cur[...].reshape(keys_tot // 8, 8, rows) - shift[None])
        total = jnp.sum(jnp.sum(prob, axis=0), axis=0, keepdims=True)
        out_v = jnp.dot(vtall[la], prob.reshape(keys_tot, rows).astype(BF16), preferred_element_type=F32)
        scores(la, nxt, s_nxt, m_nxt)
        put(obuf.at[unit], [tuple(val[:, h * ctok:(h + 1) * ctok] for val in (out_v, peak, total)) for h in range(2)])

    def before(la):
        acts = {}

        def add(name, *fns):
            acts.setdefault(SLOT[name] - 1, []).extend(fns)

        for hp in range(PAIRS):
            lw, rw = rc_qr[la][hp].wait_recv, rc_ql[la][hp].wait_recv
            fwd = rc_qf[la][hp]
            if hp % 2 == 0:
                acts.setdefault(FORWARD_BEFORE[hp], []).extend([lw, fwd.start])
                add("right%d" % hp, rw)
            else:
                acts.setdefault(FORWARD_BEFORE[hp], []).extend([rw, fwd.start])
                add("left%d" % hp, lw)
        for hp in range(PAIRS):
            add("opp%d" % hp, rc_qf[la][hp].wait_recv)
        return acts

    def after(la):
        acts = {}
        for name, cp in rc_o[la].items():
            hp = int(name[-1])
            merge_it = (name.startswith("right") and hp % 2 == 0) or (name.startswith("left") and hp % 2 == 1)

            def act(name=name, cp=cp, hp=hp, merge_it=merge_it):
                if name.startswith("left" if hp % 2 == 0 else "right"):
                    rc_qf[la][hp].wait_send()
                if merge_it:
                    rc_o[la]["opp%d" % hp].wait_recv()
                    put(obuf.at[SLOT[name]], merged_heads([obuf.at[SLOT[name]], relay.at[hp]]))
                cp.start()

            acts[SLOT[name]] = [act]
        return acts

    def attention(la):
        pl.run_scoped(functools.partial(attend_all, la), pltpu.VMEM((keys_tot, rows), F32), pltpu.VMEM((keys_tot, rows), F32),
                      *(stages if la == 0 else []))

    def attend_all(la, s_a, s_b, *next_stage):
        if next_stage:
            staged = stage_cache(1, *next_stage)
        rc_k[la].wait_recv()
        rc_v[la].wait_recv()
        with scope("score0"):
            scores(la, 0, s_a, m_a)
        pre, post = before(la), after(la)

        def run(acts, pair, parity):
            for unit, fns in acts.items():
                if unit % 2 == parity:
                    @pl.when(pair == unit // 2)
                    def _(fns=fns):
                        with scope("event"):
                            for fn in fns:
                                fn()

        def body(pair, _):
            run(pre, pair, 0)
            attend_unit(la, 2 * pair, 2 * pair + 1, s_a, m_a, s_b, m_b)
            run(post, pair, 0)
            run(pre, pair, 1)
            attend_unit(la, 2 * pair + 1, jnp.minimum(2 * pair + 2, UNITS - 1), s_b, m_b, s_a, m_a)
            run(post, pair, 1)
            return 0

        lax.fori_loop(0, UNITS // 2, body, 0)
        if next_stage:
            with scope("prep1"):
                prep_cache(1, *next_stage, staged)

    def finish_attention(la):
        for hp in range(PAIRS):
            with scope("owait"):
                rc_o[la]["right%d" % hp].wait_recv()
                rc_o[la]["left%d" % hp].wait_recv()
            heads = merged_heads([obuf.at[SLOT["own%d" % hp]], final.at[0, hp], final.at[1, hp]])
            for h, (out_v, _, total) in enumerate(heads):
                ohalf[:, pl.ds((2 * hp + h) * hd, hd)] = (out_v / total).T.astype(BF16)
        cp_wo[la].wait()
        rc_y = (rc_y1, rc_y2)[la]
        for n in range(ncol):
            ysend[n] = jnp.dot(ohalf[...], wob[:, n * cw:(n + 1) * cw], preferred_element_type=F32)
            rc_y[n].start()
        for cp in list(rc_qr[la]) + list(rc_ql[la]) + list(rc_o[la].values()):
            cp.wait_send()

    def normed(wide):
        return (wide * lax.rsqrt(jnp.mean(wide * wide, axis=-1, keepdims=True) + NORM_EPS)).astype(BF16)

    def row_loop(count, fn):
        def body(i, _):
            fn(pl.ds(pl.multiple_of(i * NORM_ROWS, NORM_ROWS), NORM_ROWS))
            return 0

        lax.fori_loop(0, count // NORM_ROWS, body, 0)

    def begin(kstage, vstage):
        cp_x.start()
        staged = stage_cache(0, kstage, vstage)
        for half in range(2):
            cp_wq[0][half].start()
        for cp in [cp_cos, cp_sin] + cp_bq + cp_bk:
            cp.start()
        cp_wk[0].start()
        cp_wv[0].start()
        with scope("entry"):
            pl.semaphore_wait(barrier, 3)
        rc_x.start()
        with scope("prep0"):
            prep_cache(0, kstage, vstage, staged)

    pl.run_scoped(begin, *stages)
    cp_cos.wait()
    cp_sin.wait()
    for cp in cp_bq + cp_bk:
        cp.wait()
    cp_x.wait()
    with scope("xwait"):
        rc_x.wait_recv()
    with scope("proj0"):
        project(0, xbuf)
    cp_wo[0].start()
    cp_wk[1].start()
    cp_wv[1].start()
    for slot in range(ff_slots):
        for cp in ff_copies(slot, slot, ff_chunk):
            cp.start()
    with scope("attn0"):
        attention(0)
    def middle(w1f, w3f, w2f):
        cols = pl.ds(pl.multiple_of(core * ff_half, 128), ff_first)
        cp_first = [local(w_gate.at[:, cols], w1f), local(w_up.at[:, cols], w3f), local(w_down.at[cols], w2f)]
        for cp in cp_first:
            cp.start()
        with scope("fin0"):
            finish_attention(0)
        with scope("ywait"):
            for n in range(ncol):
                rc_y1[n].wait()

        def first_norm(rs):
            parts = [(ysend[n, rs, :] + yrecv[n, rs, :]).astype(BF16).astype(F32) for n in range(ncol)]
            res = (xbuf[rs, :].astype(F32) + jnp.concatenate(parts, axis=1)).astype(BF16)
            hbuf[rs, :] = res
            ubuf[rs, :] = normed(res.astype(F32))

        with scope("norm1"):
            row_loop(ctok, first_norm)

        def gate_up(w1, w3):
            gate = jnp.dot(ubuf[...], w1[...], preferred_element_type=F32).astype(BF16).astype(F32)
            up = jnp.dot(ubuf[...], w3[...], preferred_element_type=F32).astype(BF16).astype(F32)
            return (jax.nn.silu(gate) * up).astype(BF16)

        def down(w2, size, send=False):
            for n in range(ncol):
                part = jnp.dot(ebuf[:, pl.ds(0, size)], w2[:, pl.ds(n * cw, cw)], preferred_element_type=F32)
                macc[n] += part
                if send:
                    rc_m[n].start()

        def ring_up(slot, size):
            return gate_up(w1s.at[slot, :, pl.ds(0, size)], w3s.at[slot, :, pl.ds(0, size)])

        def ring_down(slot, size):
            down(w2s.at[slot, pl.ds(0, size)], size)

        def refill(chunk, which):
            @pl.when(chunk < nfull)
            def _():
                cps = ff_copies(chunk, lax.rem(chunk, ff_slots), ff_chunk)
                for w in which:
                    cps[w].start()

        with scope("mlp_a"):
            macc[...] = jnp.zeros(macc.shape, F32)
            ready = ff_copies(0, 0, ff_chunk)
            ready[0].wait()
            ready[1].wait()
            ebuf[:, pl.ds(0, ff_chunk)] = ring_up(0, ff_chunk)
            refill(jnp.int32(ff_slots), (0, 1))

        def mlp_body(k, _):
            slot, prev = lax.rem(k, ff_slots), lax.rem(k - 1, ff_slots)
            cps = ff_copies(k, slot, ff_chunk)
            with scope("stream"):
                cps[0].wait()
                cps[1].wait()
                ff_copies(k - 1, prev, ff_chunk)[2].wait()
            hidden = ring_up(slot, ff_chunk)
            ring_down(prev, ff_chunk)
            ebuf[:, pl.ds(0, ff_chunk)] = hidden
            refill(k + ff_slots, (0, 1))
            refill(k - 1 + ff_slots, (2,))
            return 0

        with scope("mlp"):
            lax.fori_loop(1, nfull, mlp_body, 0)
        for half in range(2):
            cp_wq[1][half].start()
        cp_wo[1].start()
        last_slot = (nfull - 1) % ff_slots
        with scope("mlp_z"):
            ff_copies(nfull - 1, last_slot, ff_chunk)[2].wait()
            for cp in cp_first:
                cp.wait()
            hidden = gate_up(w1f, w3f)
            ring_down(last_slot, ff_chunk)
            ebuf[:, pl.ds(0, ff_first)] = hidden
            down(w2f, ff_first, send=True)
        with scope("mwait"):
            for n in range(ncol):
                rc_m[n].wait()

        def second_norm(rs):
            acc = jnp.concatenate([macc[n, rs, :] + mrecv[n, rs, :] for n in range(ncol)], axis=1)
            res = (hbuf[rs, :].astype(F32) + acc).astype(BF16)
            hbuf[rs, :] = res
            ubuf[rs, :] = normed(res.astype(F32))

        with scope("norm2"):
            row_loop(ctok, second_norm)
        gout[0] = hbuf[my_rows, :]
        cp_g.start()

    pl.run_scoped(middle, pltpu.VMEM((width, ff_first), BF16), pltpu.VMEM((width, ff_first), BF16),
                  pltpu.VMEM((ff_first, width), BF16))
    with scope("proj1"):
        project(1, ubuf)
    with scope("attn1"):
        attention(1)
    with scope("fin1"):
        finish_attention(1)
    for n in range(ncol):
        rc_y2[n].wait()
        gout[1, :, pl.ds(n * cw, cw)] = (ysend[n, my_rows, :] + yrecv[n, pl.ds(0, tok), :]).astype(BF16)
        cp_y[n].start()
    rc_x.wait_send()
    rc_k[1].wait_send()
    rc_v[1].wait_send()
    for cp in cp_kout + cp_vout + cp_y + [cp_g]:
        cp.wait()


def copy_out(*refs):
    half = len(refs) // 2
    for src, dst in zip(refs[:half], refs[half:]):
        dst[...] = src[...]


def solution(mesh):
    axis_size = mesh.shape["cp"]
    nchip = axis_size // 2
    ff_first, ff_chunk, ff_slots = 896, 512, 5
    rows_spec = P(("dp", "cp"), None)
    cache_spec = P(("dp", "cp"), None, None)
    mat_spec = P(None, None)
    vec_spec = P(None)
    layer_specs = (cache_spec, cache_spec, mat_spec, vec_spec, mat_spec, vec_spec, mat_spec, mat_spec)
    in_specs = (rows_spec,) + layer_specs + (mat_spec, mat_spec, mat_spec) + layer_specs
    out_specs = (rows_spec, rows_spec, cache_spec, cache_spec, cache_spec, cache_spec)

    def forward(x_in, cache_k1, cache_v1, w_q1, b_q1, w_k1, b_k1, w_v1, w_o1, w_gate, w_up, w_down,
                cache_k2, cache_v2, w_q2, b_q2, w_k2, b_k2, w_v2, w_o2):
        tok, width = x_in.shape
        cache_dev, kv_heads, hd = cache_k1.shape
        ctok = 2 * tok
        rows = 2 * ctok
        keys_tot = 2 * cache_dev + ctok
        cos_t, sin_t = rope_tables(axis_size * cache_dev, axis_size * tok, hd)
        flat = lambda arr: arr.reshape(-1, hd)
        half_w = width // 2
        ncol = 4
        hbm = pl.BlockSpec(memory_space=pl.ANY)
        scratch = [
            pltpu.VMEM((ctok, width), BF16),
            pltpu.VMEM((ctok, width), BF16),
            pltpu.VMEM((ctok, width), BF16),
            pltpu.VMEM((width, 4 * hd), BF16),
            pltpu.VMEM((half_w, width), BF16),
            pltpu.VMEM((2, keys_tot, hd), BF16),
            pltpu.VMEM((2, hd, keys_tot), BF16),
            pltpu.VMEM((cache_dev, hd), BF16),
            pltpu.VMEM((hd, cache_dev), BF16),
            pltpu.VMEM((8 * hd, hd), F32),
            pltpu.VMEM((UNITS, rows, hd), BF16),
            pltpu.VMEM((8, rows), F32),
            pltpu.VMEM((8, rows), F32),
            pltpu.VMEM((UNITS, 2 * hd + 8, ctok), F32),
            pltpu.VMEM((PAIRS, 2 * hd + 8, ctok), F32),
            pltpu.VMEM((2, PAIRS, 2 * hd + 8, ctok), F32),
            pltpu.VMEM((ctok, half_w), BF16),
            pltpu.VMEM((ncol, ctok, width // ncol), F32),
            pltpu.VMEM((ncol, ctok, width // ncol), F32),
            pltpu.VMEM((ncol, ctok, width // ncol), F32),
            pltpu.VMEM((ff_slots, width, ff_chunk), BF16),
            pltpu.VMEM((ff_slots, width, ff_chunk), BF16),
            pltpu.VMEM((ff_slots, ff_chunk, width), BF16),
            pltpu.VMEM((ctok, max(ff_first, ff_chunk)), BF16),
            pltpu.VMEM((ctok, hd), F32),
            pltpu.VMEM((ctok, hd), F32),
            pltpu.VMEM((2, width // hd, hd), BF16),
            pltpu.VMEM((2, kv_heads, hd), BF16),
            pltpu.VMEM((2, 2, 2 * tok, hd), BF16),
            pltpu.VMEM((2, tok, width), BF16),
            pltpu.SemaphoreType.DMA((35,)),
            pltpu.SemaphoreType.DMA((3, ff_slots)),
            pltpu.SemaphoreType.DMA((65,)),
            pltpu.SemaphoreType.DMA((65,)),
        ]
        act = jax.ShapeDtypeStruct((tok, width), BF16)
        app = jax.ShapeDtypeStruct((kv_heads * tok, hd), BF16)
        outs = pl.pallas_call(
            functools.partial(block_kernel, nchip, ff_first, ff_chunk, ff_slots),
            out_shape=(act, act, app, app, app, app),
            in_specs=[hbm] * 22,
            out_specs=(hbm,) * 6,
            scratch_shapes=scratch,
            compiler_params=pltpu.CompilerParams(collective_id=0, has_side_effects=True, vmem_limit_bytes=67043328),
        )(x_in, flat(cache_k1), flat(cache_v1), w_q1, w_k1, w_v1, w_o1, w_gate, w_up, w_down,
          flat(cache_k2), flat(cache_v2), w_q2, w_k2, w_v2, w_o2,
          flat(b_q1), flat(b_k1), flat(b_q2), flat(b_k2), jnp.asarray(cos_t), jnp.asarray(sin_t))
        outs = pl.pallas_call(copy_out, out_shape=[jax.ShapeDtypeStruct(arr.shape, arr.dtype) for arr in outs])(*outs)
        hidden, y_two = outs[:2]
        appends = [arr.reshape(tok, kv_heads, hd) for arr in outs[2:]]
        return (hidden, y_two, *appends)

    return jax.shard_map(forward, mesh=mesh, in_specs=in_specs, out_specs=out_specs, check_vma=False)
```

```python
import functools
import math

import jax
import jax.numpy as jnp
import numpy as np
from jax import lax
from jax.experimental import pallas as pl
from jax.experimental.pallas import tpu as pltpu
from jax.sharding import PartitionSpec as P

ROPE_THETA = 500000.0
NORM_EPS = 1e-5
MESH = pl.DeviceIdType.MESH
scope = jax.named_scope
F32 = jnp.float32
BF16 = jnp.bfloat16

ORDER = ("own0", "own1", "left0", "right1", "left2", "opp0", "opp1", "right3", "opp2", "opp3",
         "right0", "left1", "own2", "right2", "left3", "own3")
FORWARD_BEFORE = (1, 2, 3, 4)
SLOT = {name: idx for idx, name in enumerate(ORDER)}
UNITS = len(ORDER)
PAIRS = 4
NORM_ROWS = 64


def rope_tables(first_pos, count, head_dim):
    half_dim = head_dim // 2
    exponent = np.arange(half_dim, dtype=np.float32) * np.float32(2.0 / head_dim)
    inv_freq = (np.float32(1.0) / np.power(np.float32(ROPE_THETA), exponent)).astype(np.float32)
    positions = (first_pos + np.arange(count)).astype(np.float32)
    angles = (positions[:, None] * inv_freq[None, :]).astype(np.float32)
    cos_t = np.cos(angles.astype(np.float64)).astype(np.float32)
    sin_t = np.sin(angles.astype(np.float64)).astype(np.float32)
    return np.concatenate([cos_t, cos_t], axis=1), np.concatenate([-sin_t, sin_t], axis=1)


def block_kernel(nchip, ff_first, ff_chunk, ff_slots,
                 x_hbm, kc1, vc1, wq1, wk1, wv1, wo1, w_gate, w_up, w_down, kc2, vc2, wq2, wk2, wv2, wo2,
                 bq1, bk1, bq2, bk2, cos_hbm, sin_hbm,
                 g_out, y_out, k1_out, v1_out, k2_out, v2_out,
                 xbuf, hbuf, ubuf, wkvb, wob, kall, vtall, ksend, vsend, deint,
                 qall, m_a, m_b, obuf, relay, final, ohalf, ysend, yrecv, mrecv,
                 w1s, w3s, w2s, ebuf, cosb, sinb, bqb, bkb, kvout, gout,
                 dsem, rings, ssem, rsem):
    tok = x_hbm.shape[0]
    ctok = 2 * tok
    width = x_hbm.shape[1]
    hd = kc1.shape[1]
    keys_dev = kc1.shape[0] // 2
    keys_chip = 2 * keys_dev
    keys_tot = keys_chip + ctok
    rows = 2 * ctok
    half_w = width // 2
    ncol = 4
    cw = width // ncol
    cexp = math.log2(math.e) / math.sqrt(hd)

    me = lax.axis_index("cp")
    chip = me // 2
    core = lax.rem(me, 2)
    partner = chip * 2 + 1 - core
    left_chip = lax.rem(chip + nchip - 1, nchip)
    right_chip = lax.rem(chip + 1, nchip)
    opp_chip = lax.rem(chip + 2, nchip)
    left = left_chip * 2 + core
    right = right_chip * 2 + core

    macc = ysend
    dcount = [0]

    def local(src, dst):
        idx = dcount[0]
        dcount[0] += 1
        return pltpu.make_async_copy(src, dst, dsem.at[idx])

    rcount = [0]

    def remote(src, dst, dev):
        idx = rcount[0]
        rcount[0] += 1
        return pltpu.make_async_remote_copy(src_ref=src, dst_ref=dst, send_sem=ssem.at[idx], recv_sem=rsem.at[idx],
                                            device_id={"cp": dev}, device_id_type=MESH)

    barrier = pltpu.get_barrier_semaphore()
    for dev in (partner, left, right):
        pl.semaphore_signal(barrier, inc=1, device_id={"cp": dev}, device_id_type=MESH)

    my_rows = pl.ds(pl.multiple_of(core * tok, tok), tok)
    kc = (kc1, kc2)
    vc = (vc1, vc2)
    wq = (wq1, wq2)
    wk = (wk1, wk2)
    wv = (wv1, wv2)
    wo = (wo1, wo2)
    k_out = (k1_out, k2_out)
    v_out = (v1_out, v2_out)

    cp_x = local(x_hbm, xbuf.at[my_rows])
    pos_rows = pl.ds(pl.multiple_of(chip * ctok, ctok), ctok)
    cp_cos = local(cos_hbm.at[pos_rows], cosb)
    cp_sin = local(sin_hbm.at[pos_rows], sinb)
    cp_bq = [local(ref, bqb.at[la]) for la, ref in enumerate((bq1, bq2))]
    cp_bk = [local(ref, bkb.at[la]) for la, ref in enumerate((bk1, bk2))]
    qcol = [pl.ds(pl.multiple_of(core * half_w + half * 2 * rows, rows), 2 * rows) for half in range(2)]
    wqb = [ref.at[ff_slots - 1, :, pl.ds(0, 2 * rows)] for ref in (w1s, w3s)]
    cp_wq = [[local(wq[la].at[:, qcol[half]], wqb[half]) for half in range(2)] for la in range(2)]
    cp_wk = [local(wk[la], wkvb.at[:, pl.ds(0, 2 * hd)]) for la in range(2)]
    cp_wv = [local(wv[la], wkvb.at[:, pl.ds(2 * hd, 2 * hd)]) for la in range(2)]
    cp_wo = [local(wo[la].at[pl.ds(pl.multiple_of(core * half_w, half_w), half_w)], wob) for la in range(2)]
    cp_kout = [local(kvout.at[la, 0], k_out[la]) for la in range(2)]
    cp_vout = [local(kvout.at[la, 1], v_out[la]) for la in range(2)]
    cp_g = local(gout.at[0], g_out)
    cp_y = [local(gout.at[1, :, pl.ds(n * cw, cw)], y_out.at[:, pl.ds(n * cw, cw)]) for n in range(ncol)]

    rc_x = remote(xbuf.at[my_rows], xbuf.at[my_rows], partner)
    rc_k = [remote(ksend, kall.at[la, pl.ds(keys_dev, keys_dev)], partner) for la in range(2)]
    rc_v = [remote(vsend, vtall.at[la, :, pl.ds(keys_dev, keys_dev)], partner) for la in range(2)]
    rc_qr, rc_ql, rc_qf, rc_o = [], [], [], []
    for la in range(2):
        own = [qall.at[SLOT["own%d" % hp]] for hp in range(PAIRS)]
        rc_qr.append([remote(own[hp], qall.at[SLOT["left%d" % hp]], right) for hp in range(PAIRS)])
        rc_ql.append([remote(own[hp], qall.at[SLOT["right%d" % hp]], left) for hp in range(PAIRS)])
        fwd = []
        for hp in range(PAIRS):
            side, dev = ("left", right) if hp % 2 == 0 else ("right", left)
            fwd.append(remote(qall.at[SLOT["%s%d" % (side, hp)]], qall.at[SLOT["opp%d" % hp]], dev))
        rc_qf.append(fwd)
        outs = {}
        for hp in range(PAIRS):
            outs["left%d" % hp] = remote(obuf.at[SLOT["left%d" % hp]], final.at[1, hp], left)
            outs["right%d" % hp] = remote(obuf.at[SLOT["right%d" % hp]], final.at[0, hp], right)
            outs["opp%d" % hp] = remote(obuf.at[SLOT["opp%d" % hp]], relay.at[hp], right if hp % 2 == 0 else left)
        rc_o.append(outs)
    rc_y1 = [remote(ysend.at[n], yrecv.at[n], partner) for n in range(ncol)]
    other_rows = pl.ds(pl.multiple_of((1 - core) * tok, tok), tok)
    rc_y2 = [remote(ysend.at[n, other_rows], yrecv.at[n, pl.ds(0, tok)], partner) for n in range(ncol)]
    rc_m = [remote(macc.at[n], mrecv.at[n], partner) for n in range(ncol)]

    ff_half = w_gate.shape[1] // 2
    nfull = (ff_half - ff_first) // ff_chunk
    assert ff_half == ff_first + nfull * ff_chunk and nfull > ff_slots

    def ff_copies(chunk, slot, size):
        cols = pl.ds(pl.multiple_of(core * ff_half + ff_first + chunk * ff_chunk, 128), size)
        return (pltpu.make_async_copy(w_gate.at[:, cols], w1s.at[slot, :, pl.ds(0, size)], rings.at[0, slot]),
                pltpu.make_async_copy(w_up.at[:, cols], w3s.at[slot, :, pl.ds(0, size)], rings.at[1, slot]),
                pltpu.make_async_copy(w_down.at[cols], w2s.at[slot, pl.ds(0, size)], rings.at[2, slot]))

    def rope(val, la_bias, cos_v, sin_v):
        val = (val + la_bias).astype(BF16).astype(F32)
        return (val * cos_v + pltpu.roll(val, hd // 2, 1) * sin_v).astype(BF16)

    stages = [pltpu.VMEM(kc1.shape, BF16), pltpu.VMEM(vc1.shape, BF16)]

    def stage_cache(la, kstage, vstage):
        cps = local(kc[la], kstage), local(vc[la], vstage)
        for cp in cps:
            cp.start()
        return cps

    def prep_cache(la, kstage, vstage, cps):
        if la == 1:
            rc_k[0].wait_send()
            rc_v[0].wait_send()
        blk = deint.shape[0] // 2

        def split(ref, i):
            deint[...] = ref[pl.ds(pl.multiple_of(i * 2 * blk, 2 * blk), 2 * blk), :].astype(F32)
            head0 = deint[pl.ds(0, blk, stride=2), :]
            head1 = deint[pl.ds(1, blk, stride=2), :]
            is0 = core == 0
            return jnp.where(is0, head0, head1), jnp.where(is0, head1, head0)

        def kbody(i, _):
            mine, other = split(kstage, i)
            at = pl.ds(pl.multiple_of(i * blk, blk), blk)
            kall[la, at, :] = mine.astype(BF16)
            ksend[at, :] = other.astype(BF16)
            return 0

        def vbody(i, _):
            mine, other = split(vstage, i)
            at = pl.ds(pl.multiple_of(i * blk, blk), blk)
            vtall[la, :, at] = mine.T.astype(BF16)
            vsend[:, at] = other.T.astype(BF16)
            return 0

        cps[0].wait()
        lax.fori_loop(0, keys_dev // blk, kbody, 0)
        rc_k[la].start()
        cps[1].wait()
        lax.fori_loop(0, keys_dev // blk, vbody, 0)
        rc_v[la].start()

    def project(la, in_ref):
        heads_half = half_w // hd
        bq_v = bqb[la].astype(F32)
        bq_v = jnp.where(core == 0, bq_v[:heads_half], bq_v[heads_half:])
        bk_v = bkb[la].astype(F32)
        cos_v, sin_v = cosb[...], sinb[...]
        for half in range(2):
            cp_wq[la][half].wait()
            acc = jnp.dot(in_ref[...], wqb[half][...], preferred_element_type=F32)
            for hp in (2 * half, 2 * half + 1):
                slot = SLOT["own%d" % hp]
                for j in range(2):
                    row = hp * 2 + j
                    at = (row - 4 * half) * hd
                    qall[slot, pl.ds(j * ctok, ctok), :] = rope(acc[:, at:at + hd], bq_v[row:row + 1], cos_v, sin_v)
                rc_qr[la][hp].start()
                rc_ql[la][hp].start()
        cp_wk[la].wait()
        cp_wv[la].wait()
        acc = jnp.dot(in_ref[...], wkvb[...], preferred_element_type=F32)
        k_heads = [rope(acc[:, j * hd:(j + 1) * hd], bk_v[j:j + 1], cos_v, sin_v).astype(F32) for j in range(2)]
        acc = acc[:, 2 * hd:]
        v_heads = [acc[:, j * hd:(j + 1) * hd].astype(BF16).astype(F32) for j in range(2)]
        is0 = core == 0
        kall[la, pl.ds(keys_chip, ctok), :] = jnp.where(is0, k_heads[0], k_heads[1]).astype(BF16)
        vtall[la, :, pl.ds(keys_chip, ctok)] = jnp.where(is0, v_heads[0], v_heads[1]).T.astype(BF16)
        for which, heads in ((0, k_heads), (1, v_heads)):
            for j in range(2):
                mine = jnp.where(is0, heads[j][:tok], heads[j][tok:])
                deint[pl.ds(j, tok, stride=2), :] = mine
            kvout[la, which] = deint[pl.ds(0, 2 * tok), :].astype(BF16)
        cp_kout[la].start()
        cp_vout[la].start()

    offs = {"own": 0, "left": (left_chip - chip) * ctok, "right": (right_chip - chip) * ctok, "opp": (opp_chip - chip) * ctok}

    def unit_offset(unit):
        res = jnp.int32(0)
        for name, idx in SLOT.items():
            if not name.startswith("own"):
                res = jnp.where(unit == idx, offs[name[:-1]], res)
        return res

    def scores(la, unit, s_ref, m_ref):
        s_val = lax.dot_general(kall[la], qall[unit], (((1,), (1,)), ((), ())), preferred_element_type=F32) * cexp
        s_ref[pl.ds(0, keys_chip), :] = s_val[:keys_chip]
        peak = jnp.max(s_val[:keys_chip].reshape(keys_chip // 8, 8, rows), axis=0)
        key_i = lax.broadcasted_iota(jnp.int32, (ctok, rows), 0)
        tok_i = lax.broadcasted_iota(jnp.int32, (ctok, rows), 1) % ctok
        masked = jnp.where(key_i - tok_i <= unit_offset(unit), s_val[keys_chip:], -jnp.inf)
        s_ref[pl.ds(keys_chip, ctok), :] = masked
        m_ref[...] = jnp.maximum(peak, jnp.max(masked.reshape(ctok // 8, 8, rows), axis=0))

    row8 = lax.broadcasted_iota(jnp.int32, (8, ctok), 0)

    def put(dst, heads):
        for h, (out_v, _, _) in enumerate(heads):
            dst[pl.ds(h * hd, hd), :] = out_v
        (_, peak0, total0), (_, peak1, total1) = heads
        dst[pl.ds(2 * hd, 8), :] = jnp.where(row8 == 0, peak0, jnp.where(row8 == 1, peak1, jnp.where(row8 == 2, total0, total1)))

    def get(src):
        return [(src[pl.ds(h * hd, hd), :], src[pl.ds(2 * hd + h, 1), :], src[pl.ds(2 * hd + 2 + h, 1), :]) for h in range(2)]

    def merged(parts):
        peak = functools.reduce(jnp.maximum, [part[1] for part in parts])
        scales = [jnp.exp2(part[1] - peak) for part in parts]
        out_v = functools.reduce(jnp.add, [part[0] * sc for part, sc in zip(parts, scales)])
        total = functools.reduce(jnp.add, [part[2] * sc for part, sc in zip(parts, scales)])
        return out_v, peak, total

    def merged_heads(refs):
        return [merged(parts) for parts in zip(*[get(ref) for ref in refs])]

    def attend_unit(la, unit, nxt, s_cur, m_cur, s_nxt, m_nxt):
        peak = jnp.max(m_cur[...], axis=0, keepdims=True)
        shift = jnp.broadcast_to(peak, (8, rows))
        prob = jnp.exp2(s_cur[...].reshape(keys_tot // 8, 8, rows) - shift[None])
        total = jnp.sum(jnp.sum(prob, axis=0), axis=0, keepdims=True)
        out_v = jnp.dot(vtall[la], prob.reshape(keys_tot, rows).astype(BF16), preferred_element_type=F32)
        scores(la, nxt, s_nxt, m_nxt)
        put(obuf.at[unit], [tuple(val[:, h * ctok:(h + 1) * ctok] for val in (out_v, peak, total)) for h in range(2)])

    def before(la):
        acts = {}

        def add(name, *fns):
            acts.setdefault(SLOT[name] - 1, []).extend(fns)

        for hp in range(PAIRS):
            lw, rw = rc_qr[la][hp].wait_recv, rc_ql[la][hp].wait_recv
            fwd = rc_qf[la][hp]
            if hp % 2 == 0:
                acts.setdefault(FORWARD_BEFORE[hp], []).extend([lw, fwd.start])
                add("right%d" % hp, rw)
            else:
                acts.setdefault(FORWARD_BEFORE[hp], []).extend([rw, fwd.start])
                add("left%d" % hp, lw)
        for hp in range(PAIRS):
            add("opp%d" % hp, rc_qf[la][hp].wait_recv)
        return acts

    def after(la):
        acts = {}
        for name, cp in rc_o[la].items():
            hp = int(name[-1])
            merge_it = (name.startswith("right") and hp % 2 == 0) or (name.startswith("left") and hp % 2 == 1)

            def act(name=name, cp=cp, hp=hp, merge_it=merge_it):
                if name.startswith("left" if hp % 2 == 0 else "right"):
                    rc_qf[la][hp].wait_send()
                if merge_it:
                    rc_o[la]["opp%d" % hp].wait_recv()
                    put(obuf.at[SLOT[name]], merged_heads([obuf.at[SLOT[name]], relay.at[hp]]))
                cp.start()

            acts[SLOT[name]] = [act]
        return acts

    def attention(la):
        pl.run_scoped(functools.partial(attend_all, la), pltpu.VMEM((keys_tot, rows), F32), pltpu.VMEM((keys_tot, rows), F32),
                      *(stages if la == 0 else []))

    def attend_all(la, s_a, s_b, *next_stage):
        if next_stage:
            staged = stage_cache(1, *next_stage)
        rc_k[la].wait_recv()
        rc_v[la].wait_recv()
        with scope("score0"):
            scores(la, 0, s_a, m_a)
        pre, post = before(la), after(la)

        def run(acts, pair, parity):
            for unit, fns in acts.items():
                if unit % 2 == parity:
                    @pl.when(pair == unit // 2)
                    def _(fns=fns):
                        with scope("event"):
                            for fn in fns:
                                fn()

        def body(pair, _):
            run(pre, pair, 0)
            attend_unit(la, 2 * pair, 2 * pair + 1, s_a, m_a, s_b, m_b)
            run(post, pair, 0)
            run(pre, pair, 1)
            attend_unit(la, 2 * pair + 1, jnp.minimum(2 * pair + 2, UNITS - 1), s_b, m_b, s_a, m_a)
            run(post, pair, 1)
            return 0

        lax.fori_loop(0, UNITS // 2, body, 0)
        if next_stage:
            with scope("prep1"):
                prep_cache(1, *next_stage, staged)

    def finish_attention(la):
        for hp in range(PAIRS):
            with scope("owait"):
                rc_o[la]["right%d" % hp].wait_recv()
                rc_o[la]["left%d" % hp].wait_recv()
            heads = merged_heads([obuf.at[SLOT["own%d" % hp]], final.at[0, hp], final.at[1, hp]])
            for h, (out_v, _, total) in enumerate(heads):
                ohalf[:, pl.ds((2 * hp + h) * hd, hd)] = (out_v / total).T.astype(BF16)
        cp_wo[la].wait()
        rc_y = (rc_y1, rc_y2)[la]
        for n in range(ncol):
            ysend[n] = jnp.dot(ohalf[...], wob[:, n * cw:(n + 1) * cw], preferred_element_type=F32)
            rc_y[n].start()
        for cp in list(rc_qr[la]) + list(rc_ql[la]) + list(rc_o[la].values()):
            cp.wait_send()

    def normed(wide):
        return (wide * lax.rsqrt(jnp.mean(wide * wide, axis=-1, keepdims=True) + NORM_EPS)).astype(BF16)

    def row_loop(count, fn):
        def body(i, _):
            fn(pl.ds(pl.multiple_of(i * NORM_ROWS, NORM_ROWS), NORM_ROWS))
            return 0

        lax.fori_loop(0, count // NORM_ROWS, body, 0)

    def begin(kstage, vstage):
        cp_x.start()
        staged = stage_cache(0, kstage, vstage)
        for half in range(2):
            cp_wq[0][half].start()
        for cp in [cp_cos, cp_sin] + cp_bq + cp_bk:
            cp.start()
        cp_wk[0].start()
        cp_wv[0].start()
        with scope("entry"):
            pl.semaphore_wait(barrier, 3)
            cp_x.wait()
        rc_x.start()
        with scope("prep0"):
            prep_cache(0, kstage, vstage, staged)

    pl.run_scoped(begin, *stages)
    cp_cos.wait()
    cp_sin.wait()
    for cp in cp_bq + cp_bk:
        cp.wait()
    with scope("xwait"):
        rc_x.wait_recv()
    with scope("proj0"):
        project(0, xbuf)
    cp_wo[0].start()
    cp_wk[1].start()
    cp_wv[1].start()
    for slot in range(ff_slots):
        for cp in ff_copies(slot, slot, ff_chunk):
            cp.start()
    with scope("attn0"):
        attention(0)
    def middle(w1f, w3f, w2f):
        cols = pl.ds(pl.multiple_of(core * ff_half, 128), ff_first)
        cp_first = [local(w_gate.at[:, cols], w1f), local(w_up.at[:, cols], w3f), local(w_down.at[cols], w2f)]
        for cp in cp_first:
            cp.start()
        with scope("fin0"):
            finish_attention(0)
        with scope("ywait"):
            for n in range(ncol):
                rc_y1[n].wait()

        def first_norm(rs):
            parts = [(ysend[n, rs, :] + yrecv[n, rs, :]).astype(BF16).astype(F32) for n in range(ncol)]
            res = (xbuf[rs, :].astype(F32) + jnp.concatenate(parts, axis=1)).astype(BF16)
            hbuf[rs, :] = res
            ubuf[rs, :] = normed(res.astype(F32))

        with scope("norm1"):
            row_loop(ctok, first_norm)

        def gate_up(w1, w3):
            gate = jnp.dot(ubuf[...], w1[...], preferred_element_type=F32).astype(BF16).astype(F32)
            up = jnp.dot(ubuf[...], w3[...], preferred_element_type=F32).astype(BF16).astype(F32)
            return (jax.nn.silu(gate) * up).astype(BF16)

        def down(w2, size, send=False):
            for n in range(ncol):
                part = jnp.dot(ebuf[:, pl.ds(0, size)], w2[:, pl.ds(n * cw, cw)], preferred_element_type=F32)
                macc[n] += part
                if send:
                    rc_m[n].start()

        def ring_up(slot, size):
            return gate_up(w1s.at[slot, :, pl.ds(0, size)], w3s.at[slot, :, pl.ds(0, size)])

        def ring_down(slot, size):
            down(w2s.at[slot, pl.ds(0, size)], size)

        def refill(chunk, which):
            @pl.when(chunk < nfull)
            def _():
                cps = ff_copies(chunk, lax.rem(chunk, ff_slots), ff_chunk)
                for w in which:
                    cps[w].start()

        with scope("mlp_a"):
            macc[...] = jnp.zeros(macc.shape, F32)
            ready = ff_copies(0, 0, ff_chunk)
            ready[0].wait()
            ready[1].wait()
            ebuf[:, pl.ds(0, ff_chunk)] = ring_up(0, ff_chunk)
            refill(jnp.int32(ff_slots), (0, 1))

        def mlp_body(k, _):
            slot, prev = lax.rem(k, ff_slots), lax.rem(k - 1, ff_slots)
            cps = ff_copies(k, slot, ff_chunk)
            with scope("stream"):
                cps[0].wait()
                cps[1].wait()
                ff_copies(k - 1, prev, ff_chunk)[2].wait()
            hidden = ring_up(slot, ff_chunk)
            ring_down(prev, ff_chunk)
            ebuf[:, pl.ds(0, ff_chunk)] = hidden
            refill(k + ff_slots, (0, 1))
            refill(k - 1 + ff_slots, (2,))
            return 0

        with scope("mlp"):
            lax.fori_loop(1, nfull, mlp_body, 0)
        for half in range(2):
            cp_wq[1][half].start()
        cp_wo[1].start()
        last_slot = (nfull - 1) % ff_slots
        with scope("mlp_z"):
            ff_copies(nfull - 1, last_slot, ff_chunk)[2].wait()
            for cp in cp_first:
                cp.wait()
            hidden = gate_up(w1f, w3f)
            ring_down(last_slot, ff_chunk)
            ebuf[:, pl.ds(0, ff_first)] = hidden
            down(w2f, ff_first, send=True)
        with scope("mwait"):
            for n in range(ncol):
                rc_m[n].wait()

        def second_norm(rs):
            acc = jnp.concatenate([macc[n, rs, :] + mrecv[n, rs, :] for n in range(ncol)], axis=1)
            res = (hbuf[rs, :].astype(F32) + acc).astype(BF16)
            hbuf[rs, :] = res
            ubuf[rs, :] = normed(res.astype(F32))

        with scope("norm2"):
            row_loop(ctok, second_norm)
        gout[0] = hbuf[my_rows, :]
        cp_g.start()

    pl.run_scoped(middle, pltpu.VMEM((width, ff_first), BF16), pltpu.VMEM((width, ff_first), BF16),
                  pltpu.VMEM((ff_first, width), BF16))
    with scope("proj1"):
        project(1, ubuf)
    with scope("attn1"):
        attention(1)
    with scope("fin1"):
        finish_attention(1)
    for n in range(ncol):
        rc_y2[n].wait()
        gout[1, :, pl.ds(n * cw, cw)] = (ysend[n, my_rows, :] + yrecv[n, pl.ds(0, tok), :]).astype(BF16)
        cp_y[n].start()
    rc_x.wait_send()
    rc_k[1].wait_send()
    rc_v[1].wait_send()
    for cp in cp_kout + cp_vout + cp_y + [cp_g]:
        cp.wait()


def copy_out(*refs):
    half = len(refs) // 2
    for src, dst in zip(refs[:half], refs[half:]):
        dst[...] = src[...]


def solution(mesh):
    axis_size = mesh.shape["cp"]
    nchip = axis_size // 2
    ff_first, ff_chunk, ff_slots = 896, 512, 5
    rows_spec = P(("dp", "cp"), None)
    cache_spec = P(("dp", "cp"), None, None)
    mat_spec = P(None, None)
    vec_spec = P(None)
    layer_specs = (cache_spec, cache_spec, mat_spec, vec_spec, mat_spec, vec_spec, mat_spec, mat_spec)
    in_specs = (rows_spec,) + layer_specs + (mat_spec, mat_spec, mat_spec) + layer_specs
    out_specs = (rows_spec, rows_spec, cache_spec, cache_spec, cache_spec, cache_spec)

    def forward(x_in, cache_k1, cache_v1, w_q1, b_q1, w_k1, b_k1, w_v1, w_o1, w_gate, w_up, w_down,
                cache_k2, cache_v2, w_q2, b_q2, w_k2, b_k2, w_v2, w_o2):
        tok, width = x_in.shape
        cache_dev, kv_heads, hd = cache_k1.shape
        ctok = 2 * tok
        rows = 2 * ctok
        keys_tot = 2 * cache_dev + ctok
        cos_t, sin_t = rope_tables(axis_size * cache_dev, axis_size * tok, hd)
        flat = lambda arr: arr.reshape(-1, hd)
        half_w = width // 2
        ncol = 4
        hbm = pl.BlockSpec(memory_space=pl.ANY)
        scratch = [
            pltpu.VMEM((ctok, width), BF16),
            pltpu.VMEM((ctok, width), BF16),
            pltpu.VMEM((ctok, width), BF16),
            pltpu.VMEM((width, 4 * hd), BF16),
            pltpu.VMEM((half_w, width), BF16),
            pltpu.VMEM((2, keys_tot, hd), BF16),
            pltpu.VMEM((2, hd, keys_tot), BF16),
            pltpu.VMEM((cache_dev, hd), BF16),
            pltpu.VMEM((hd, cache_dev), BF16),
            pltpu.VMEM((8 * hd, hd), F32),
            pltpu.VMEM((UNITS, rows, hd), BF16),
            pltpu.VMEM((8, rows), F32),
            pltpu.VMEM((8, rows), F32),
            pltpu.VMEM((UNITS, 2 * hd + 8, ctok), F32),
            pltpu.VMEM((PAIRS, 2 * hd + 8, ctok), F32),
            pltpu.VMEM((2, PAIRS, 2 * hd + 8, ctok), F32),
            pltpu.VMEM((ctok, half_w), BF16),
            pltpu.VMEM((ncol, ctok, width // ncol), F32),
            pltpu.VMEM((ncol, ctok, width // ncol), F32),
            pltpu.VMEM((ncol, ctok, width // ncol), F32),
            pltpu.VMEM((ff_slots, width, ff_chunk), BF16),
            pltpu.VMEM((ff_slots, width, ff_chunk), BF16),
            pltpu.VMEM((ff_slots, ff_chunk, width), BF16),
            pltpu.VMEM((ctok, max(ff_first, ff_chunk)), BF16),
            pltpu.VMEM((ctok, hd), F32),
            pltpu.VMEM((ctok, hd), F32),
            pltpu.VMEM((2, width // hd, hd), BF16),
            pltpu.VMEM((2, kv_heads, hd), BF16),
            pltpu.VMEM((2, 2, 2 * tok, hd), BF16),
            pltpu.VMEM((2, tok, width), BF16),
            pltpu.SemaphoreType.DMA((35,)),
            pltpu.SemaphoreType.DMA((3, ff_slots)),
            pltpu.SemaphoreType.DMA((65,)),
            pltpu.SemaphoreType.DMA((65,)),
        ]
        act = jax.ShapeDtypeStruct((tok, width), BF16)
        app = jax.ShapeDtypeStruct((kv_heads * tok, hd), BF16)
        outs = pl.pallas_call(
            functools.partial(block_kernel, nchip, ff_first, ff_chunk, ff_slots),
            out_shape=(act, act, app, app, app, app),
            in_specs=[hbm] * 22,
            out_specs=(hbm,) * 6,
            scratch_shapes=scratch,
            compiler_params=pltpu.CompilerParams(collective_id=0, has_side_effects=True, vmem_limit_bytes=67043328),
        )(x_in, flat(cache_k1), flat(cache_v1), w_q1, w_k1, w_v1, w_o1, w_gate, w_up, w_down,
          flat(cache_k2), flat(cache_v2), w_q2, w_k2, w_v2, w_o2,
          flat(b_q1), flat(b_k1), flat(b_q2), flat(b_k2), jnp.asarray(cos_t), jnp.asarray(sin_t))
        outs = pl.pallas_call(copy_out, out_shape=[jax.ShapeDtypeStruct(arr.shape, arr.dtype) for arr in outs])(*outs)
        hidden, y_two = outs[:2]
        appends = [arr.reshape(tok, kv_heads, hd) for arr in outs[2:]]
        return (hidden, y_two, *appends)

    return jax.shard_map(forward, mesh=mesh, in_specs=in_specs, out_specs=out_specs, check_vma=False)
```
